256 devices in a mesh: leaf: 64 (over z, y, core), panel: 4 (over x).
Axes of the slice: x: 4, y: 4, z: 8, core: 2. Of those that a mesh axis runs over, the one named last changes fastest.
Arguments:
- subtree_solution: bfloat16 [32, 4, 131072], P(None, 'panel', 'leaf'), may hold values from -6 to 6
- subtree_coupling: bfloat16 [4, 8192, 2048], P('panel', 'leaf'), may hold values from -0.25 to 0.25
- sub_map: int32 [4, 8192], P('panel', 'leaf'), may hold values from 0 to 8191
- sub_count: int32 [4, 64], P('panel', 'leaf'), may hold values from 1 to 128, 4096 in all within a row
- front_rhs: float32 [32, 4, 8192], P(None, 'panel', 'leaf'), may hold values from -6 to 6
- sep_inverse: bfloat16 [4, 8192, 8192], P('panel', None, 'leaf'), may hold values from -0.0625 to 0.0625
- border_coupling: bfloat16 [4, 8192, 2048], P('panel', 'leaf'), may hold values from -0.0625 to 0.0625
- border_map: int32 [4, 2048], replicated, may hold values from 0 to 10239
- root_rhs: float32 [32, 10240], P(None, 'panel'), may hold values from -6 to 6
- root_inverse: bfloat16 [10240, 10240], P('leaf', 'panel'), may hold values from -0.0625 to 0.0625
Outputs:
- root_forward: float32 [32, 10240], P(None, 'leaf')
- root_solution: float32 [32, 10240], P(None, 'panel')
- front_solution: float32 [32, 4, 8192], P(None, 'panel', 'leaf')
- subtree_update: float32 [32, 4, 131072], P(None, 'panel', 'leaf')
The draws below stay inside these ranges and needn't reach their ends.
Inputs may be any that keep to these rules, and one draw needn't show every extreme that they name: `sub_map`: only the first sub_count entries of a subtree's rows are live. `sub_count`: over one front's 64 subtrees the counts sum to 4096.
All inputs are finite; a program needn't handle non-finite values. No bound on the sum of `sub_count` on one device may be relied on, other than what follows from the above.
Results may differ from the reference program's by a relative error of at most 0.0075.
Values may be sent and summed in bfloat16 or wider, within the bound.
No kernel may reach another device: no remote copies, remote signals or barrier semaphores. Data moves between devices by JAX's collectives and lax.ppermute only.
A program may use at most 64 MiB of HBM per device.

```python
import math
import jax
import jax.numpy as jnp
import numpy as np

RHS_COUNT = 32
S1 = 10240
S2 = 8192
E2 = 2048
SUBTREE_TOP_ROWS = 2048
COUPLING_ROWS = 128
LEVEL_TWO_FRONTS = 4
N_LEAF = 64


def with_ends(array, stream_key, low, high):
    extent = array.shape
    spot = [jax.random.randint(jax.random.fold_in(stream_key, axis), (), 0, extent[axis]) for axis in range(len(extent))]
    array = array.at[tuple(spot)].set(low)
    longest = extent.index(max(extent))
    spot[longest] = (spot[longest] + 1) % extent[longest]
    return array.at[tuple(spot)].set(high)


def levels(stream_key, shape, pieces, least, largest):
    loudness, own = 1.0, jax.random.fold_in(stream_key, 6)
    for axis_at, parts in pieces:
        draws = jnp.exp(jax.random.uniform(jax.random.fold_in(own, axis_at), (parts,), jnp.float32, least / len(pieces), largest / len(pieces)))
        loudness = loudness * jnp.repeat(draws, shape[axis_at] // parts).reshape([-1 if axis == axis_at else 1 for axis in range(len(shape))])
    return loudness


def profile(amount, total, bound, lean):
    weights = [(1 << 20) // math.isqrt(standing ** lean) + 1 for standing in range(2, amount + 1)]
    surplus, given = total - bound - (amount - 1), [1] * (amount - 1)
    while surplus > 0:
        movable = [i for i in range(amount - 1) if given[i] < bound]
        mass, left = sum([weights[i] for i in movable]), surplus
        for i in movable:
            extra = min(bound - given[i], max(1, left * weights[i] // mass), surplus)
            given[i] = given[i] + extra
            surplus = surplus - extra
    return np.array([bound] + given)


def uneven(rng, number_of, total, limit, slope):
    if number_of == 2:
        one = jax.random.randint(rng, (), max(1, total - limit), min(limit, total - 1) + 1)
        return jnp.stack([one, total - one])
    tallies = jnp.asarray(profile(number_of, total, limit, slope), jnp.int32)
    couples = (number_of - 1) // 2
    giver, sink = tallies[1:1 + 2 * couples:2], tallies[2:2 + 2 * couples:2]
    room = jnp.minimum(giver - 1, limit - sink)
    passed = jax.random.randint(jax.random.fold_in(rng, 1), (couples,), 0, 1 << 20) % (room + 1)
    tallies = tallies.at[1:1 + 2 * couples:2].set(giver - passed).at[2:2 + 2 * couples:2].set(sink + passed)
    return tallies[jax.random.permutation(jax.random.fold_in(rng, 2), number_of)]


def normal_values(stream_key, extent, spread, limit, shards=(), kind=jnp.bfloat16):
    result = spread * jax.random.normal(stream_key, extent, jnp.float32)
    if shards:
        result = result * levels(stream_key, extent, shards, -0.22, 0.18)
    return jnp.clip(result, -limit, limit).astype(kind)


def setup_inputs(seed: int = 0) -> dict:
    arg_keys = jax.random.split(jax.random.key(seed), 11)
    return {
        "subtree_solution": normal_values(arg_keys[0], (RHS_COUNT, LEVEL_TWO_FRONTS, N_LEAF * SUBTREE_TOP_ROWS), 1.0, 6.0, ((1, 4), (2, 64))),
        "subtree_coupling": normal_values(arg_keys[1], (LEVEL_TWO_FRONTS, N_LEAF * COUPLING_ROWS, SUBTREE_TOP_ROWS), (SUBTREE_TOP_ROWS // 4) ** -0.5, 0.25, ((0, 4), (1, 64))),
        "sub_map": with_ends(jax.random.randint(arg_keys[2], (LEVEL_TWO_FRONTS, N_LEAF * COUPLING_ROWS), 0, S2), jax.random.fold_in(arg_keys[2], 1), 0, S2 - 1).astype(jnp.int32),
        "sub_count": jax.vmap(lambda own: uneven(own, N_LEAF, N_LEAF * COUPLING_ROWS // 2, COUPLING_ROWS, 2))(jax.random.split(arg_keys[3], LEVEL_TWO_FRONTS)).reshape((LEVEL_TWO_FRONTS, N_LEAF)).astype(jnp.int32),
        "front_rhs": normal_values(arg_keys[4], (RHS_COUNT, LEVEL_TWO_FRONTS, S2), 1.0, 6.0, ((1, 4), (2, 64)), jnp.float32),
        "sep_inverse": normal_values(arg_keys[5], (LEVEL_TWO_FRONTS, S2, S2), S2 ** -0.5, 0.0625, ((0, 4), (2, 64))),
        "border_coupling": normal_values(arg_keys[6], (LEVEL_TWO_FRONTS, S2, E2), S2 ** -0.5, 0.0625, ((0, 4), (1, 64))),
        "border_map": with_ends(jax.random.randint(arg_keys[7], (LEVEL_TWO_FRONTS, E2), 0, S1), jax.random.fold_in(arg_keys[7], 1), 0, S1 - 1).astype(jnp.int32),
        "root_rhs": normal_values(arg_keys[8], (RHS_COUNT, S1), 1.0, 6.0, ((1, 4),), jnp.float32),
        "root_inverse": normal_values(arg_keys[9], (S1, S1), S1 ** -0.5, 0.0625, ((0, 64), (1, 4))),
    }


def reference(subtree_solution, subtree_coupling, sub_map, sub_count, front_rhs, sep_inverse, border_coupling, border_map, root_rhs, root_inverse):
    positions = jnp.arange(COUPLING_ROWS, dtype=jnp.int32)
    forward_list = []
    border_list = []
    coupling_factors = []
    living_list = []
    for front_index in range(LEVEL_TWO_FRONTS):
        solved_values = subtree_solution[:, front_index, :].reshape(RHS_COUNT, N_LEAF, SUBTREE_TOP_ROWS).astype(jnp.float32)
        coupling_factor = subtree_coupling[front_index].reshape(N_LEAF, COUPLING_ROWS, SUBTREE_TOP_ROWS).astype(jnp.float32)
        living = positions[None, :] < sub_count[front_index][:, None]
        contrib = jnp.einsum("rls,ljs->rlj", solved_values, coupling_factor)
        contrib = jnp.where(living[None, :, :], contrib, jnp.zeros_like(contrib))
        extended = jnp.zeros((RHS_COUNT, S2), jnp.float32).at[:, sub_map[front_index]].add(contrib.reshape(RHS_COUNT, N_LEAF * COUPLING_ROWS))
        assembled = (front_rhs[:, front_index, :] - extended).astype(jnp.bfloat16)
        forward = jnp.dot(assembled, sep_inverse[front_index].T, preferred_element_type=jnp.float32)
        border_term = jnp.dot(forward.astype(jnp.bfloat16), border_coupling[front_index], preferred_element_type=jnp.float32)
        forward_list.append(forward)
        border_list.append(border_term)
        coupling_factors.append(coupling_factor)
        living_list.append(living)
    border_all = jnp.stack(border_list, axis=1).reshape(RHS_COUNT, LEVEL_TWO_FRONTS * E2)
    root_term = jnp.zeros((RHS_COUNT, S1), jnp.float32).at[:, border_map.reshape(-1)].add(border_all)
    root_assembled = (root_rhs - root_term).astype(jnp.bfloat16)
    root_forward = jnp.dot(root_assembled, root_inverse.T, preferred_element_type=jnp.float32)
    root_solution = jnp.dot(root_forward.astype(jnp.bfloat16), root_inverse, preferred_element_type=jnp.float32)
    root_half = root_solution.astype(jnp.bfloat16)
    solution_list = []
    update_list = []
    for front_index in range(LEVEL_TWO_FRONTS):
        picked = root_half[:, border_map[front_index]]
        residual = forward_list[front_index] - jnp.dot(picked, border_coupling[front_index].T, preferred_element_type=jnp.float32)
        solution = jnp.dot(residual.astype(jnp.bfloat16), sep_inverse[front_index], preferred_element_type=jnp.float32)
        front_half = solution.astype(jnp.bfloat16)
        gathered_values = front_half[:, sub_map[front_index]].reshape(RHS_COUNT, N_LEAF, COUPLING_ROWS).astype(jnp.float32)
        gathered_values = jnp.where(living_list[front_index][None, :, :], gathered_values, jnp.zeros_like(gathered_values))
        update_term = jnp.einsum("fvq,vqo->fvo", gathered_values, coupling_factors[front_index]).reshape(RHS_COUNT, N_LEAF * SUBTREE_TOP_ROWS)
        solution_list.append(solution)
        update_list.append(update_term)
    front_solution = jnp.stack(solution_list, axis=1)
    subtree_update = jnp.stack(update_list, axis=1)
    return root_forward, root_solution, front_solution, subtree_update
```

```python
import jax
import jax.numpy as jnp
from jax import lax
from jax.experimental import pallas as pl
from jax.experimental.pallas import tpu as pltpu
from jax.sharding import Mesh
from jax.sharding import PartitionSpec as P

LEAF = ("z", "y", "c")
F32, BF16 = jnp.float32, jnp.bfloat16
NT = (((1,), (1,)), ((), ()))
NN = (((1,), (0,)), ((), ()))


def mm(a, b, dims=NN):
    return lax.dot_general(a, b, dims, preferred_element_type=F32)


def smem():
    return pl.BlockSpec(memory_space=pltpu.SMEM)


def vmem():
    return pl.BlockSpec(memory_space=pltpu.VMEM)


def kernel_call(body, outs, n_smem, n_vmem, flops=0, name=None):
    return pl.pallas_call(
        body,
        out_shape=outs,
        in_specs=[smem()] * n_smem + [vmem()] * n_vmem,
        out_specs=jax.tree.map(lambda _: vmem(), outs),
        cost_estimate=pl.CostEstimate(flops=flops, bytes_accessed=flops // 64, transcendentals=0) if flops else None,
        name=name,
    )


def like(shape, dtype):
    return jax.ShapeDtypeStruct(shape, dtype)


def scatter_kernel(at, count, solved, coupling, sub_map, keep, send):
    c = at[0]
    contrib = mm(solved[...], coupling[...], NT)
    lane = lax.broadcasted_iota(jnp.int32, (1, 128), 1)
    live = lane < count[0, 0]
    contrib = jnp.where(live, contrib, 0.0)
    high = contrib.astype(BF16)
    low = (contrib - high.astype(F32)).astype(BF16)
    both = jnp.concatenate([high, low], axis=0)
    rows = jnp.where(live, sub_map[...], -1)
    batch = contrib.shape[0]
    iota = lax.broadcasted_iota(jnp.int32, (256, 128), 0)
    for block in range(keep.shape[0]):
        hot = jnp.where(iota == rows - block * 256, 1.0, 0.0).astype(BF16)
        spread = mm(both, hot, NT)
        spread = spread[:batch] + spread[batch:]
        first, second = spread[:, :128], spread[:, 128:]
        keep[block] = jnp.where(c == 0, first, second)
        send[block] = jnp.where(c == 0, second, first).astype(BF16)


def forward_kernel(at, arrived, rhs, slab, keep, send):
    c = at[0]
    total = jnp.sum(arrived[...].astype(F32), axis=0)
    assembled = (rhs[...] - total).astype(BF16)
    for block in range(keep.shape[0]):
        part = mm(assembled, slab[block * 256 : (block + 1) * 256, :], NT)
        first, second = part[:, :128], part[:, 128:]
        keep[block] = jnp.where(c == 0, first, second)
        send[block] = jnp.where(c == 0, second, first).astype(BF16)


def fold_kernel(base, border, columns, out):
    width = 256
    cols = columns[...]
    lane = lax.broadcasted_iota(jnp.int32, (1, 128), 1)
    left = border[...]
    for block in range(out.shape[1] // width):
        start = base + block * width
        halves = [
            jnp.where(cols == lane + (start + half * 128), 1.0, 0.0).astype(BF16)
            for half in range(width // 128)
        ]
        hot = jnp.concatenate(halves, axis=1)
        out[:, block * width : (block + 1) * width] = mm(left, hot).astype(BF16)


def border_kernel(at, arrived, b0, b1, b2, b3, forward, keep, send):
    c = at[0]
    total = jnp.sum(arrived[...].astype(F32), axis=0)
    forward[...] = total
    half = total.astype(BF16)
    width = keep.shape[2]
    for y in range(4):
        for x, folded in enumerate((b0, b1, b2, b3)):
            part = mm(half, folded[:, y * width : (y + 1) * width])
            first, second = part[:16], part[16:]
            keep[y * 4 + x] = jnp.where(c == 0, first, second)
            send[y * 4 + x] = jnp.where(c == 0, second, first).astype(BF16)


def pick(index, items):
    out = items[0]
    for k, item in enumerate(items[1:], 1):
        out = jnp.where(index == k, item, out)
    return out


def root_forward_kernel(at, own, other, inverse, out):
    c, y = at[0], at[1]
    width = own.shape[2]
    total = None
    for there in range(4):
        k = lax.rem(y - there + 4, 4)
        mine, theirs = own[k], other[k]
        first = jnp.where(c == 0, mine, theirs)
        second = jnp.where(c == 0, theirs, mine)
        left = jnp.concatenate([first, second], axis=0)
        part = mm(left, inverse[:, there * width : (there + 1) * width], NT)
        total = part if total is None else total + part
    out[...] = total


def root_back_kernel(at, p0, p1, p2, p3, inverse, forward, keep, send):
    c, y, x = at[0], at[1], at[2]
    parts = (p0[...], p1[...], p2[...], p3[...])
    total = None
    for panel in range(4):
        part = pick(lax.rem(x - panel + 4, 4), parts)
        total = part if total is None else total + part
    forward[...] = total
    half = total.astype(BF16)
    width = keep.shape[2]
    for there in range(4):
        k = lax.rem(there - y + 4, 4)
        part = mm(half, inverse[:, there * width : (there + 1) * width])
        first, second = part[:16], part[16:]
        keep[k] = jnp.where(c == 0, first, second)
        send[k] = jnp.where(c == 0, second, first).astype(BF16)


def residual_kernel(at, own, other, b0, b1, b2, b3, forward, residual, solution):
    c, x_at = at[0], at[2]
    width = own.shape[2]
    total = forward[...]
    for y in range(4):
        for x, folded in enumerate((b0, b1, b2, b3)):
            mine, theirs = own[y * 4 + x], other[y * 4 + x]
            first = jnp.where(c == 0, mine, theirs)
            second = jnp.where(c == 0, theirs, mine)
            left = jnp.concatenate([first, second], axis=0)
            total = total - mm(left, folded[:, y * width : (y + 1) * width], NT)
        mine, theirs = own[y * 4 + x_at], other[y * 4 + x_at]
        cols = slice(y * width, (y + 1) * width)
        solution[:16, cols] = jnp.where(c == 0, mine, theirs).astype(F32)
        solution[16:, cols] = jnp.where(c == 0, theirs, mine).astype(F32)
    residual[...] = total.astype(BF16)


def front_kernel(at, own, other, slab, out, half):
    c = at[0]
    total = None
    for block in range(own.shape[0]):
        mine, theirs = own[block], other[block]
        first = jnp.where(c == 0, mine, theirs)
        second = jnp.where(c == 0, theirs, mine)
        left = jnp.concatenate([first, second], axis=1)
        part = mm(left, slab[block * 256 : (block + 1) * 256, :])
        total = part if total is None else total + part
    out[:, 0, :] = total
    half[...] = total.astype(BF16)


def update_kernel(at, count, own, other, sub_map, coupling, out):
    c = at[0]
    lane = lax.broadcasted_iota(jnp.int32, (1, 128), 1)
    rows = jnp.where(lane < count[0, 0], sub_map[...], -1)
    iota = lax.broadcasted_iota(jnp.int32, (256, 128), 0)
    total = None
    for block in range(own.shape[0]):
        mine, theirs = own[block], other[block]
        first = jnp.where(c == 0, mine, theirs)
        second = jnp.where(c == 0, theirs, mine)
        left = jnp.concatenate([first, second], axis=1)
        hot = jnp.where(iota == rows - block * 256, 1.0, 0.0).astype(BF16)
        part = mm(left, hot)
        total = part if total is None else total + part
    out[:, 0, :] = mm(total.astype(BF16), coupling[...])


def swap_core(x):
    return lax.ppermute(x, "c", [(0, 1), (1, 0)])


def shifted(x, axis, k):
    return lax.ppermute(x, axis, [(i, (i + k) % 4) for i in range(4)])


def exchange(x, axes):
    return lax.all_to_all(x, axes, split_axis=0, concat_axis=0, tiled=True)


def to_everyone(x, axes, peers):
    return exchange(jnp.broadcast_to(x, (peers, *x.shape)), axes)


def joined(keep, got):
    return keep + got.astype(F32)


def body(
    subtree_solution,
    subtree_coupling,
    sub_map,
    sub_count,
    front_rhs,
    sep_inverse,
    border_coupling,
    border_map,
    root_rhs,
    root_inverse,
):
    z_size, y_size = lax.axis_size("z"), lax.axis_size("y")
    peers = z_size * y_size
    c, y, x = lax.axis_index("c"), lax.axis_index("y"), lax.axis_index("x")
    at = jnp.stack([c, y, x]).astype(jnp.int32)
    solved = subtree_solution[:, 0, :]
    coupling = subtree_coupling[0]
    slab = sep_inverse[0]
    border = border_coupling[0]
    batch = solved.shape[0]
    split = like((peers, batch, 128), F32), like((peers, batch, 128), BF16)

    own_map = lax.dynamic_index_in_dim(border_map, x, 0, keepdims=False)
    columns = jnp.broadcast_to(own_map[:, None], (own_map.shape[0], 128))
    panel_width = root_rhs.shape[1]
    folded = []
    for panel in range(4):
        call = kernel_call(
            lambda b, k, o, base=panel * panel_width: fold_kernel(base, b, k, o),
            like((border.shape[0], panel_width), BF16),
            0,
            2,
            flops=2 * border.shape[0] * border.shape[1] * panel_width,
            name=f"fold{panel}",
        )
        folded.append(call(border, columns))

    keep, send = kernel_call(scatter_kernel, split, 2, 3, name="scatter")(
        at, sub_count, solved, coupling, sub_map
    )
    arrived = exchange(joined(keep, swap_core(send)).astype(BF16), ("z", "y"))
    keep, send = kernel_call(forward_kernel, split, 1, 3, name="forward")(
        at, arrived, front_rhs[:, 0, :], slab
    )
    arrived = exchange(joined(keep, swap_core(send)).astype(BF16), ("z", "y"))

    quarter = panel_width // 4
    forward, keep, send = kernel_call(
        border_kernel,
        (like((batch, 128), F32), like((16, 16, quarter), F32), like((16, 16, quarter), BF16)),
        1,
        5,
        name="border",
    )(at, arrived, *folded)
    arrived = exchange(joined(keep, swap_core(send)).astype(BF16), ("y", "x"))
    near = arrived.astype(F32).sum(axis=0).astype(BF16)
    border_sum = to_everyone(near, "z", z_size).astype(F32).sum(axis=0)
    rhs_part = lax.dynamic_slice(root_rhs, (c * 16, y * quarter), (16, quarter))
    chunk = (rhs_part - border_sum).astype(BF16)
    own = jnp.stack([chunk] + [shifted(chunk, "y", k) for k in (1, 2, 3)])
    partial = kernel_call(
        root_forward_kernel, like((batch, root_inverse.shape[0]), F32), 1, 3, name="rootf"
    )(at, own, swap_core(own), root_inverse)

    parts = [partial] + [shifted(partial, "x", k) for k in (1, 2, 3)]
    root_forward, keep, send = kernel_call(
        root_back_kernel,
        (
            like((batch, root_inverse.shape[0]), F32),
            like((4, 16, quarter), F32),
            like((4, 16, quarter), BF16),
        ),
        1,
        5,
        name="rootb",
    )(at, *parts, root_inverse)
    col = joined(keep, swap_core(send))
    near = col[0]
    for k in (1, 2, 3):
        near = near + shifted(col[k].astype(BF16), "y", k).astype(F32)
    chunk = to_everyone(near.astype(BF16), "z", z_size).astype(F32).sum(axis=0).astype(BF16)
    own = to_everyone(chunk, ("y", "x"), 16)
    residual, root_solution = kernel_call(
        residual_kernel,
        (like((batch, 128), BF16), like((batch, panel_width), F32)),
        1,
        7,
        name="resid",
    )(at, own, swap_core(own), *folded, forward)

    own = to_everyone(residual, ("z", "y"), peers)
    front_solution, front_half = kernel_call(
        front_kernel, (like((batch, 1, 128), F32), like((batch, 128), BF16)), 1, 3, name="front"
    )(at, own, swap_core(own), slab)
    own = to_everyone(front_half, ("z", "y"), peers)
    subtree_update = kernel_call(
        update_kernel, like((batch, 1, coupling.shape[1]), F32), 2, 4, name="update"
    )(at, sub_count, own, swap_core(own), sub_map, coupling)
    return (root_forward, root_solution, front_solution, subtree_update)


def solution(mesh):
    finer = Mesh(mesh.devices.reshape(8, 4, 2, mesh.shape["panel"]), ("z", "y", "c", "x"))
    in_specs = (
        P(None, "x", LEAF),
        P("x", LEAF, None),
        P("x", LEAF),
        P("x", LEAF),
        P(None, "x", LEAF),
        P("x", None, LEAF),
        P("x", LEAF, None),
        P(None, None),
        P(None, "x"),
        P(LEAF, "x"),
    )
    out_specs = (P(None, LEAF), P(None, "x"), P(None, "x", LEAF), P(None, "x", LEAF))
    return jax.shard_map(
        body, mesh=finer, in_specs=in_specs, out_specs=out_specs, check_vma=False
    )
```

```python
import jax
import jax.numpy as jnp
from jax import lax
from jax.experimental import pallas as pl
from jax.experimental.pallas import tpu as pltpu
from jax.sharding import Mesh
from jax.sharding import PartitionSpec as P

LEAF = ("z", "y", "c")
F32, BF16 = jnp.float32, jnp.bfloat16
NT = (((1,), (1,)), ((), ()))
NN = (((1,), (0,)), ((), ()))


def mm(a, b, dims=NN):
    return lax.dot_general(a, b, dims, preferred_element_type=F32)


def smem():
    return pl.BlockSpec(memory_space=pltpu.SMEM)


def vmem():
    return pl.BlockSpec(memory_space=pltpu.VMEM)


def kernel_call(body, outs, n_smem, n_vmem, flops=0, name=None, near=(), near_out=()):
    flat, tree = jax.tree.flatten(outs)
    flat = [pltpu.VMEM(o.shape, o.dtype) if i in near_out else o for i, o in enumerate(flat)]
    call = pl.pallas_call(
        body,
        out_shape=jax.tree.unflatten(tree, flat),
        in_specs=[smem()] * n_smem + [vmem()] * n_vmem,
        out_specs=jax.tree.map(lambda _: vmem(), outs),
        cost_estimate=pl.CostEstimate(flops=flops, bytes_accessed=flops // 64, transcendentals=0) if flops else None,
        name=name,
    )

    def run(*args):
        args = list(args)
        for i in near:
            args[n_smem + i] = pltpu.with_memory_space_constraint(args[n_smem + i], pltpu.VMEM)
        return call(*args)

    return run


def like(shape, dtype):
    return jax.ShapeDtypeStruct(shape, dtype)


def scatter_kernel(at, count, solved, coupling, sub_map, keep, send):
    c = at[0]
    contrib = mm(solved[...], coupling[...], NT)
    lane = lax.broadcasted_iota(jnp.int32, (1, 128), 1)
    live = lane < count[0, 0]
    contrib = jnp.where(live, contrib, 0.0)
    high = contrib.astype(BF16)
    low = (contrib - high.astype(F32)).astype(BF16)
    both = jnp.concatenate([high, low], axis=0)
    rows = jnp.where(live, sub_map[...], -1)
    batch = contrib.shape[0]
    iota = lax.broadcasted_iota(jnp.int32, (256, 128), 0)
    for block in range(keep.shape[0]):
        hot = jnp.where(iota == rows - block * 256, 1.0, 0.0).astype(BF16)
        spread = mm(both, hot, NT)
        spread = spread[:batch] + spread[batch:]
        first, second = spread[:, :128], spread[:, 128:]
        keep[block] = jnp.where(c == 0, first, second)
        send[block] = jnp.where(c == 0, second, first).astype(BF16)


def forward_kernel(at, arrived, rhs, slab, keep, send):
    c = at[0]
    total = jnp.sum(arrived[...].astype(F32), axis=0)
    assembled = (rhs[...] - total).astype(BF16)
    for block in range(keep.shape[0]):
        part = mm(assembled, slab[block * 256 : (block + 1) * 256, :], NT)
        first, second = part[:, :128], part[:, 128:]
        keep[block] = jnp.where(c == 0, first, second)
        send[block] = jnp.where(c == 0, second, first).astype(BF16)


def fold_kernel(base, border, columns, out):
    width = 256
    cols = columns[...]
    lane = lax.broadcasted_iota(jnp.int32, (1, 128), 1)
    left = border[...]
    for block in range(out.shape[1] // width):
        start = base + block * width
        halves = [
            jnp.where(cols == lane + (start + half * 128), 1.0, 0.0).astype(BF16)
            for half in range(width // 128)
        ]
        hot = jnp.concatenate(halves, axis=1)
        out[:, block * width : (block + 1) * width] = mm(left, hot).astype(BF16)


def border_kernel(at, arrived, b0, b1, b2, b3, forward, keep, send):
    c = at[0]
    total = jnp.sum(arrived[...].astype(F32), axis=0)
    forward[...] = total
    half = total.astype(BF16)
    width = keep.shape[2]
    for y in range(4):
        for x, folded in enumerate((b0, b1, b2, b3)):
            part = mm(half, folded[:, y * width : (y + 1) * width])
            first, second = part[:16], part[16:]
            keep[y * 4 + x] = jnp.where(c == 0, first, second)
            send[y * 4 + x] = jnp.where(c == 0, second, first).astype(BF16)


def pick(index, items):
    out = items[0]
    for k, item in enumerate(items[1:], 1):
        out = jnp.where(index == k, item, out)
    return out


def root_forward_kernel(at, own, other, inverse, out):
    c, y = at[0], at[1]
    width = own.shape[2]
    total = None
    for there in range(4):
        k = lax.rem(y - there + 4, 4)
        mine, theirs = own[k], other[k]
        first = jnp.where(c == 0, mine, theirs)
        second = jnp.where(c == 0, theirs, mine)
        left = jnp.concatenate([first, second], axis=0)
        part = mm(left, inverse[:, there * width : (there + 1) * width], NT)
        total = part if total is None else total + part
    out[...] = total


def root_back_kernel(at, p0, p1, p2, p3, inverse, forward, keep, send):
    c, y, x = at[0], at[1], at[2]
    parts = (p0[...], p1[...], p2[...], p3[...])
    total = None
    for panel in range(4):
        part = pick(lax.rem(x - panel + 4, 4), parts)
        total = part if total is None else total + part
    forward[...] = total
    half = total.astype(BF16)
    width = keep.shape[2]
    for there in range(4):
        k = lax.rem(there - y + 4, 4)
        part = mm(half, inverse[:, there * width : (there + 1) * width])
        first, second = part[:16], part[16:]
        keep[k] = jnp.where(c == 0, first, second)
        send[k] = jnp.where(c == 0, second, first).astype(BF16)


def residual_kernel(at, own, other, b0, b1, b2, b3, forward, residual, solution):
    c, x_at = at[0], at[2]
    width = own.shape[2]
    total = forward[...]
    for y in range(4):
        for x, folded in enumerate((b0, b1, b2, b3)):
            mine, theirs = own[y * 4 + x], other[y * 4 + x]
            first = jnp.where(c == 0, mine, theirs)
            second = jnp.where(c == 0, theirs, mine)
            left = jnp.concatenate([first, second], axis=0)
            total = total - mm(left, folded[:, y * width : (y + 1) * width], NT)
        mine, theirs = own[y * 4 + x_at], other[y * 4 + x_at]
        cols = slice(y * width, (y + 1) * width)
        solution[:16, cols] = jnp.where(c == 0, mine, theirs).astype(F32)
        solution[16:, cols] = jnp.where(c == 0, theirs, mine).astype(F32)
    residual[...] = total.astype(BF16)


def front_kernel(at, own, other, slab, out, half):
    c = at[0]
    total = None
    for block in range(own.shape[0]):
        mine, theirs = own[block], other[block]
        first = jnp.where(c == 0, mine, theirs)
        second = jnp.where(c == 0, theirs, mine)
        left = jnp.concatenate([first, second], axis=1)
        part = mm(left, slab[block * 256 : (block + 1) * 256, :])
        total = part if total is None else total + part
    out[:, 0, :] = total
    half[...] = total.astype(BF16)


def update_kernel(at, count, own, other, sub_map, coupling, out):
    c = at[0]
    lane = lax.broadcasted_iota(jnp.int32, (1, 128), 1)
    rows = jnp.where(lane < count[0, 0], sub_map[...], -1)
    iota = lax.broadcasted_iota(jnp.int32, (256, 128), 0)
    total = None
    for block in range(own.shape[0]):
        mine, theirs = own[block], other[block]
        first = jnp.where(c == 0, mine, theirs)
        second = jnp.where(c == 0, theirs, mine)
        left = jnp.concatenate([first, second], axis=1)
        hot = jnp.where(iota == rows - block * 256, 1.0, 0.0).astype(BF16)
        part = mm(left, hot)
        total = part if total is None else total + part
    out[:, 0, :] = mm(total.astype(BF16), coupling[...])


def swap_core(x):
    return lax.ppermute(x, "c", [(0, 1), (1, 0)])


def shifted(x, axis, k):
    return lax.ppermute(x, axis, [(i, (i + k) % 4) for i in range(4)])


def exchange(x, axes):
    return lax.all_to_all(x, axes, split_axis=0, concat_axis=0, tiled=True)


def to_everyone(x, axes, peers):
    return exchange(jnp.broadcast_to(x, (peers, *x.shape)), axes)


def joined(keep, got):
    return keep + got.astype(F32)


def body(
    subtree_solution,
    subtree_coupling,
    sub_map,
    sub_count,
    front_rhs,
    sep_inverse,
    border_coupling,
    border_map,
    root_rhs,
    root_inverse,
):
    z_size, y_size = lax.axis_size("z"), lax.axis_size("y")
    peers = z_size * y_size
    c, y, x = lax.axis_index("c"), lax.axis_index("y"), lax.axis_index("x")
    at = jnp.stack([c, y, x]).astype(jnp.int32)
    solved = subtree_solution[:, 0, :]
    coupling = subtree_coupling[0]
    slab = sep_inverse[0]
    border = border_coupling[0]
    batch = solved.shape[0]
    split = like((peers, batch, 128), F32), like((peers, batch, 128), BF16)

    own_map = lax.dynamic_index_in_dim(border_map, x, 0, keepdims=False)
    columns = jnp.broadcast_to(own_map[:, None], (own_map.shape[0], 128))
    panel_width = root_rhs.shape[1]
    folded = []
    for panel in range(4):
        call = kernel_call(
            lambda b, k, o, base=panel * panel_width: fold_kernel(base, b, k, o),
            like((border.shape[0], panel_width), BF16),
            0,
            2,
            flops=2 * border.shape[0] * border.shape[1] * panel_width,
            name=f"fold{panel}",
        )
        folded.append(call(border, columns))

    keep, send = kernel_call(scatter_kernel, split, 2, 3, name="scatter", near_out=(0, 1))(
        at, sub_count, solved, coupling, sub_map
    )
    arrived = exchange(joined(keep, swap_core(send)).astype(BF16), ("z", "y"))
    arrived, *folded[:2] = lax.optimization_barrier((arrived, *folded[:2]))
    keep, send = kernel_call(forward_kernel, split, 1, 3, name="forward", near=(0,), near_out=(0, 1))(
        at, arrived, front_rhs[:, 0, :], slab
    )
    arrived = exchange(joined(keep, swap_core(send)).astype(BF16), ("z", "y"))

    quarter = panel_width // 4
    forward, keep, send = kernel_call(
        border_kernel,
        (like((batch, 128), F32), like((16, 16, quarter), F32), like((16, 16, quarter), BF16)),
        1,
        5,
        name="border",
        near=(0,),
        near_out=(0, 1, 2),
    )(at, arrived, *folded)
    rhs_part = lax.dynamic_slice(root_rhs, (c * 16, y * quarter), (16, quarter))
    joint = joined(keep, swap_core(send)).astype(BF16)
    joint, rhs_part = lax.optimization_barrier((joint, rhs_part))
    arrived = exchange(joint, ("y", "x"))
    near = arrived.astype(F32).sum(axis=0).astype(BF16)
    border_sum = to_everyone(near, "z", z_size).astype(F32).sum(axis=0)
    chunk = (rhs_part - border_sum).astype(BF16)
    own = jnp.stack([chunk] + [shifted(chunk, "y", k) for k in (1, 2, 3)])
    partial = kernel_call(
        root_forward_kernel, like((batch, root_inverse.shape[0]), F32), 1, 3, name="rootf", near=(0, 1), near_out=(0,)
    )(at, own, swap_core(own), root_inverse)

    parts = [partial] + [shifted(partial, "x", k) for k in (1, 2, 3)]
    root_forward, keep, send = kernel_call(
        root_back_kernel,
        (
            like((batch, root_inverse.shape[0]), F32),
            like((4, 16, quarter), F32),
            like((4, 16, quarter), BF16),
        ),
        1,
        5,
        name="rootb",
        near=(0, 1, 2, 3),
        near_out=(1, 2),
    )(at, *parts, root_inverse)
    col = joined(keep, swap_core(send))
    near = col[0]
    for k in (1, 2, 3):
        near = near + shifted(col[k].astype(BF16), "y", k).astype(F32)
    chunk = to_everyone(near.astype(BF16), "z", z_size).astype(F32).sum(axis=0).astype(BF16)
    own = to_everyone(chunk, ("y", "x"), 16)
    residual, root_solution = kernel_call(
        residual_kernel,
        (like((batch, 128), BF16), like((batch, panel_width), F32)),
        1,
        7,
        name="resid",
        near=(0, 1, 6),
        near_out=(0,),
    )(at, own, swap_core(own), *folded, forward)

    own = to_everyone(residual, ("z", "y"), peers)
    front_solution, front_half = kernel_call(
        front_kernel, (like((batch, 1, 128), F32), like((batch, 128), BF16)), 1, 3, name="front", near=(0, 1), near_out=(1,)
    )(at, own, swap_core(own), slab)
    own = to_everyone(front_half, ("z", "y"), peers)
    subtree_update = kernel_call(
        update_kernel, like((batch, 1, coupling.shape[1]), F32), 2, 4, name="update", near=(0, 1)
    )(at, sub_count, own, swap_core(own), sub_map, coupling)
    return (root_forward, root_solution, front_solution, subtree_update)


def solution(mesh):
    finer = Mesh(mesh.devices.reshape(8, 4, 2, mesh.shape["panel"]), ("z", "y", "c", "x"))
    in_specs = (
        P(None, "x", LEAF),
        P("x", LEAF, None),
        P("x", LEAF),
        P("x", LEAF),
        P(None, "x", LEAF),
        P("x", None, LEAF),
        P("x", LEAF, None),
        P(None, None),
        P(None, "x"),
        P(LEAF, "x"),
    )
    out_specs = (P(None, LEAF), P(None, "x"), P(None, "x", LEAF), P(None, "x", LEAF))
    return jax.shard_map(
        body, mesh=finer, in_specs=in_specs, out_specs=out_specs, check_vma=False
    )
```

```python
import jax
import jax.numpy as jnp
from jax import lax
from jax.experimental import pallas as pl
from jax.experimental.pallas import tpu as pltpu
from jax.sharding import Mesh
from jax.sharding import PartitionSpec as P

LEAF = ("z", "y", "c")
F32, BF16 = jnp.float32, jnp.bfloat16
NT = (((1,), (1,)), ((), ()))
NN = (((1,), (0,)), ((), ()))


def mm(a, b, dims=NN):
    return lax.dot_general(a, b, dims, preferred_element_type=F32)


def smem():
    return pl.BlockSpec(memory_space=pltpu.SMEM)


def vmem():
    return pl.BlockSpec(memory_space=pltpu.VMEM)


def kernel_call(body, outs, n_smem, n_vmem, flops=0, name=None, near=(), near_out=(), stream=None, parts=0):
    stream = stream or []
    flat, tree = jax.tree.flatten(outs)
    flat = [pltpu.VMEM(o.shape, o.dtype) if i in near_out else o for i, o in enumerate(flat)]
    call = pl.pallas_call(
        body,
        out_shape=jax.tree.unflatten(tree, flat),
        in_specs=[smem()] * n_smem
        + [vmem()] * n_vmem
        + [pl.BlockSpec(memory_space=pl.ANY)] * len(stream),
        out_specs=jax.tree.map(lambda _: vmem(), outs),
        scratch_shapes=[pltpu.VMEM(x, BF16) for x in stream]
        + ([pltpu.SemaphoreType.DMA((len(stream), parts))] if stream else []),
        cost_estimate=pl.CostEstimate(flops=flops, bytes_accessed=flops // 64, transcendentals=0) if flops else None,
        name=name,
    )

    def run(*args):
        args = list(args)
        for i in near:
            args[n_smem + i] = pltpu.with_memory_space_constraint(args[n_smem + i], pltpu.VMEM)
        return call(*args)

    return run


def like(shape, dtype):
    return jax.ShapeDtypeStruct(shape, dtype)


def first_second(c, mine, theirs):
    return jnp.where(c == 0, mine, theirs), jnp.where(c == 0, theirs, mine)


def scatter_kernel(count, solved, coupling, sub_map, keep, send):
    c = lax.axis_index("c")
    contrib = mm(solved[...], coupling[...], NT)
    lane = lax.broadcasted_iota(jnp.int32, (1, 128), 1)
    live = lane < count[0, 0]
    contrib = jnp.where(live, contrib, 0.0)
    high = contrib.astype(BF16)
    low = (contrib - high.astype(F32)).astype(BF16)
    both = jnp.concatenate([high, low], axis=0)
    rows = jnp.where(live, sub_map[...], -1)
    batch = contrib.shape[0]
    iota = lax.broadcasted_iota(jnp.int32, (256, 128), 0)
    for block in range(keep.shape[0]):
        hot = jnp.where(iota == rows - block * 256, 1.0, 0.0).astype(BF16)
        spread = mm(both, hot, NT)
        spread = spread[:batch] + spread[batch:]
        first, second = spread[:, :128], spread[:, 128:]
        keep[block] = jnp.where(c == 0, first, second)
        send[block] = jnp.where(c == 0, second, first).astype(BF16)


def row_copies(source, buffer, sems, parts):
    rows = source.shape[0] // parts
    return [
        pltpu.make_async_copy(
            source.at[pl.ds(i * rows, rows), :], buffer.at[pl.ds(i * rows, rows), :], sems.at[0, i]
        )
        for i in range(parts)
    ]


def forward_kernel(arrived, rhs, source, keep, send, slab, sems):
    c = lax.axis_index("c")
    parts = 8
    copies = row_copies(source, slab, sems, parts)
    for copy in copies:
        copy.start()
    total = jnp.sum(arrived[...].astype(F32), axis=0)
    assembled = (rhs[...] - total).astype(BF16)
    per = keep.shape[0] // parts
    for block in range(keep.shape[0]):
        if block % per == 0:
            copies[block // per].wait()
        part = mm(assembled, slab[block * 256 : (block + 1) * 256, :], NT)
        first, second = part[:, :128], part[:, 128:]
        keep[block] = jnp.where(c == 0, first, second)
        send[block] = jnp.where(c == 0, second, first).astype(BF16)


def fold_kernel(base, border, columns, out):
    width = 256
    cols = columns[...]
    lane = lax.broadcasted_iota(jnp.int32, (1, 128), 1)
    left = border[...]
    for block in range(out.shape[1] // width):
        start = base + block * width
        halves = [
            jnp.where(cols == lane + (start + half * 128), 1.0, 0.0).astype(BF16)
            for half in range(width // 128)
        ]
        hot = jnp.concatenate(halves, axis=1)
        out[:, block * width : (block + 1) * width] = mm(left, hot).astype(BF16)


def fold_copies(sources, buffers, sems, width):
    return [
        [
            pltpu.make_async_copy(
                source.at[:, pl.ds(y * width, width)],
                buffer.at[:, pl.ds(y * width, width)],
                sems.at[x, y],
            )
            for x, (source, buffer) in enumerate(zip(sources, buffers))
        ]
        for y in range(4)
    ]


def border_kernel(arrived, s0, s1, s2, s3, forward, keep, send, b0, b1, b2, b3, sems):
    c = lax.axis_index("c")
    width = keep.shape[2]
    folds = (b0, b1, b2, b3)
    copies = fold_copies((s0, s1, s2, s3), folds, sems, width)
    for row in copies:
        for copy in row:
            copy.start()
    total = jnp.sum(arrived[...].astype(F32), axis=0)
    forward[...] = total
    half = total.astype(BF16)
    for y in range(4):
        for x in range(4):
            copies[y][x].wait()
            part = mm(half, folds[x][:, y * width : (y + 1) * width])
            first, second = part[:16], part[16:]
            keep[y * 4 + x] = jnp.where(c == 0, first, second)
            send[y * 4 + x] = jnp.where(c == 0, second, first).astype(BF16)


def pick(index, items):
    out = items[0]
    for k, item in enumerate(items[1:], 1):
        out = jnp.where(index == k, item, out)
    return out


def root_forward_kernel(whole, inverse, out):
    width = whole.shape[2]
    total = None
    for y in range(4):
        left = jnp.concatenate([whole[2 * y], whole[2 * y + 1]], axis=0)
        part = mm(left, inverse[:, y * width : (y + 1) * width], NT)
        total = part if total is None else total + part
    out[...] = total


def root_back_kernel(p0, p1, p2, p3, inverse, forward, out):
    x = lax.axis_index("x")
    parts = (p0[...], p1[...], p2[...], p3[...])
    total = None
    for panel in range(4):
        part = pick(lax.rem(x - panel + 4, 4), parts)
        total = part if total is None else total + part
    forward[...] = total
    half = total.astype(BF16)
    width = out.shape[2]
    for y in range(4):
        part = mm(half, inverse[:, y * width : (y + 1) * width]).astype(BF16)
        out[2 * y] = part[:16]
        out[2 * y + 1] = part[16:]


def residual_kernel(own, other, forward, s0, s1, s2, s3, residual, solution, b0, b1, b2, b3, sems):
    c, x_at = lax.axis_index("c"), lax.axis_index("x")
    width = own.shape[2]
    folds = (b0, b1, b2, b3)
    copies = fold_copies((s0, s1, s2, s3), folds, sems, width)
    for row in copies:
        for copy in row:
            copy.start()
    total = forward[...]
    for y in range(4):
        first, second = first_second(c, own[y * 4 + x_at], other[y * 4 + x_at])
        cols = slice(y * width, (y + 1) * width)
        solution[:16, cols] = first.astype(F32)
        solution[16:, cols] = second.astype(F32)
    for y in range(4):
        for x in range(4):
            left = jnp.concatenate(first_second(c, own[y * 4 + x], other[y * 4 + x]), axis=0)
            copies[y][x].wait()
            total = total - mm(left, folds[x][:, y * width : (y + 1) * width], NT)
    residual[...] = total.astype(BF16)


def front_kernel(own, other, source, out, half, slab, sems):
    c = lax.axis_index("c")
    parts = 8
    copies = row_copies(source, slab, sems, parts)
    for copy in copies:
        copy.start()
    total = None
    per = own.shape[0] // parts
    for block in range(own.shape[0]):
        left = jnp.concatenate(first_second(c, own[block], other[block]), axis=1)
        if block % per == 0:
            copies[block // per].wait()
        part = mm(left, slab[block * 256 : (block + 1) * 256, :])
        total = part if total is None else total + part
    out[:, 0, :] = total
    half[...] = total.astype(BF16)


def update_kernel(count, own, other, sub_map, coupling, out):
    c = lax.axis_index("c")
    lane = lax.broadcasted_iota(jnp.int32, (1, 128), 1)
    rows = jnp.where(lane < count[0, 0], sub_map[...], -1)
    iota = lax.broadcasted_iota(jnp.int32, (256, 128), 0)
    total = None
    for block in range(own.shape[0]):
        left = jnp.concatenate(first_second(c, own[block], other[block]), axis=1)
        hot = jnp.where(iota == rows - block * 256, 1.0, 0.0).astype(BF16)
        part = mm(left, hot)
        total = part if total is None else total + part
    out[:, 0, :] = mm(total.astype(BF16), coupling[...])


def swap_core(x):
    return lax.ppermute(x, "c", [(0, 1), (1, 0)])


def shifted(x, axis, k):
    return lax.ppermute(x, axis, [(i, (i + k) % 4) for i in range(4)])


def exchange(x, axes):
    return lax.all_to_all(x, axes, split_axis=0, concat_axis=0, tiled=True)


def to_everyone(x, axes, peers):
    return exchange(jnp.broadcast_to(x, (peers, *x.shape)), axes)


def joined(keep, got):
    return keep + got.astype(F32)


def body(
    subtree_solution,
    subtree_coupling,
    sub_map,
    sub_count,
    front_rhs,
    sep_inverse,
    border_coupling,
    border_map,
    root_rhs,
    root_inverse,
):
    z_size, y_size = lax.axis_size("z"), lax.axis_size("y")
    peers = z_size * y_size
    c, y, x = lax.axis_index("c"), lax.axis_index("y"), lax.axis_index("x")
    solved = subtree_solution[:, 0, :]
    coupling = subtree_coupling[0]
    slab = sep_inverse[0]
    border = border_coupling[0]
    batch = solved.shape[0]
    split = like((peers, batch, 128), F32), like((peers, batch, 128), BF16)

    own_map = lax.dynamic_index_in_dim(border_map, x, 0, keepdims=False)
    columns = jnp.broadcast_to(own_map[:, None], (own_map.shape[0], 128))
    panel_width = root_rhs.shape[1]
    folded = []
    for panel in range(4):
        call = kernel_call(
            lambda b, k, o, base=panel * panel_width: fold_kernel(base, b, k, o),
            like((border.shape[0], panel_width), BF16),
            0,
            2,
            flops=2 * border.shape[0] * border.shape[1] * panel_width,
            name=f"fold{panel}",
        )
        folded.append(call(border, columns))

    keep, send = kernel_call(scatter_kernel, split, 1, 3, name="scatter", near_out=(0, 1))(
        sub_count, solved, coupling, sub_map
    )
    arrived = exchange(joined(keep, swap_core(send)).astype(BF16), ("z", "y"))
    arrived, *folded[:2] = lax.optimization_barrier((arrived, *folded[:2]))
    keep, send = kernel_call(
        forward_kernel,
        split,
        0,
        2,
        name="forward",
        near=(0,),
        near_out=(0, 1),
        stream=[slab.shape],
        parts=8,
    )(arrived, front_rhs[:, 0, :], slab)
    arrived = exchange(joined(keep, swap_core(send)).astype(BF16), ("z", "y"))

    quarter = panel_width // 4
    fold_shapes = [f.shape for f in folded]
    forward, keep, send = kernel_call(
        border_kernel,
        (like((batch, 128), F32), like((16, 16, quarter), F32), like((16, 16, quarter), BF16)),
        0,
        1,
        name="border",
        near=(0,),
        near_out=(0, 1, 2),
        stream=fold_shapes,
        parts=4,
    )(arrived, *folded)
    rhs_part = lax.dynamic_slice(root_rhs, (c * 16, y * quarter), (16, quarter))
    joint = joined(keep, swap_core(send)).astype(BF16)
    joint, rhs_part = lax.optimization_barrier((joint, rhs_part))
    arrived = exchange(joint, ("y", "x"))
    near = arrived.astype(F32).sum(axis=0).astype(BF16)
    border_sum = to_everyone(near, "z", z_size).astype(F32).sum(axis=0)
    chunk = (rhs_part - border_sum).astype(BF16)
    whole = to_everyone(chunk, ("y", "c"), 8)
    partial = kernel_call(
        root_forward_kernel,
        like((batch, root_inverse.shape[0]), F32),
        0,
        2,
        name="rootf",
        near=(0, 1),
        near_out=(0,),
    )(whole, root_inverse)

    parts = [partial] + [shifted(partial, "x", k) for k in (1, 2, 3)]
    root_forward, col = kernel_call(
        root_back_kernel,
        (like((batch, root_inverse.shape[0]), F32), like((8, 16, quarter), BF16)),
        0,
        5,
        name="rootb",
        near=(0, 1, 2, 3, 4),
        near_out=(1,),
    )(*parts, root_inverse)
    near = exchange(col, ("y", "c")).astype(F32).sum(axis=0).astype(BF16)
    chunk = to_everyone(near, "z", z_size).astype(F32).sum(axis=0).astype(BF16)
    own = to_everyone(chunk, ("y", "x"), 16)
    residual, root_solution = kernel_call(
        residual_kernel,
        (like((batch, 128), BF16), like((batch, panel_width), F32)),
        0,
        3,
        name="resid",
        near=(0, 1, 2),
        near_out=(0,),
        stream=fold_shapes,
        parts=4,
    )(own, swap_core(own), forward, *folded)

    own = to_everyone(residual, ("z", "y"), peers)
    front_solution, front_half = kernel_call(
        front_kernel,
        (like((batch, 1, 128), F32), like((batch, 128), BF16)),
        0,
        2,
        name="front",
        near=(0, 1),
        near_out=(1,),
        stream=[slab.shape],
        parts=8,
    )(own, swap_core(own), slab)
    own = to_everyone(front_half, ("z", "y"), peers)
    subtree_update = kernel_call(
        update_kernel,
        like((batch, 1, coupling.shape[1]), F32),
        1,
        4,
        name="update",
        near=(0, 1, 3),
    )(sub_count, own, swap_core(own), sub_map, coupling)
    return (root_forward, root_solution, front_solution, subtree_update)


def solution(mesh):
    finer = Mesh(mesh.devices.reshape(8, 4, 2, mesh.shape["panel"]), ("z", "y", "c", "x"))
    in_specs = (
        P(None, "x", LEAF),
        P("x", LEAF, None),
        P("x", LEAF),
        P("x", LEAF),
        P(None, "x", LEAF),
        P("x", None, LEAF),
        P("x", LEAF, None),
        P(None, None),
        P(None, "x"),
        P(LEAF, "x"),
    )
    out_specs = (P(None, LEAF), P(None, "x"), P(None, "x", LEAF), P(None, "x", LEAF))
    return jax.shard_map(
        body, mesh=finer, in_specs=in_specs, out_specs=out_specs, check_vma=False
    )
```

```python
import jax
import jax.numpy as jnp
from jax import lax
from jax.experimental import pallas as pl
from jax.experimental.pallas import tpu as pltpu
from jax.sharding import Mesh
from jax.sharding import PartitionSpec as P

LEAF = ("z", "y", "c")
F32, BF16 = jnp.float32, jnp.bfloat16
NT = (((1,), (1,)), ((), ()))
NN = (((1,), (0,)), ((), ()))


def mm(a, b, dims=NN):
    return lax.dot_general(a, b, dims, preferred_element_type=F32)


def smem():
    return pl.BlockSpec(memory_space=pltpu.SMEM)


def vmem():
    return pl.BlockSpec(memory_space=pltpu.VMEM)


def kernel_call(body, outs, n_smem, n_vmem, flops=0, name=None, near=(), near_out=(), stream=(), far_out=()):
    flat, tree = jax.tree.flatten(outs)
    flat = [pltpu.VMEM(o.shape, o.dtype) if i in near_out else o for i, o in enumerate(flat)]
    call = pl.pallas_call(
        body,
        out_shape=jax.tree.unflatten(tree, flat),
        in_specs=[smem()] * n_smem
        + [vmem()] * n_vmem
        + [pl.BlockSpec(memory_space=pl.ANY)] * len(stream),
        out_specs=jax.tree.unflatten(
            tree,
            [pl.BlockSpec(memory_space=pl.ANY) if i in far_out else vmem() for i in range(len(flat))],
        ),
        scratch_shapes=[pltpu.VMEM(x, BF16) for x in stream]
        + [pltpu.VMEM(flat[i].shape, flat[i].dtype) for i in far_out]
        + [pltpu.SemaphoreType.DMA] * (len(stream) + len(far_out)),
        cost_estimate=pl.CostEstimate(flops=flops, bytes_accessed=flops // 64, transcendentals=0) if flops else None,
        name=name,
    )

    def run(*args):
        args = list(args)
        for i in near:
            args[n_smem + i] = pltpu.with_memory_space_constraint(args[n_smem + i], pltpu.VMEM)
        return call(*args)

    return run


def like(shape, dtype):
    return jax.ShapeDtypeStruct(shape, dtype)


def first_second(c, mine, theirs):
    return jnp.where(c == 0, mine, theirs), jnp.where(c == 0, theirs, mine)


def scatter_kernel(count, solved, coupling, sub_map, keep, send):
    c = lax.axis_index("c")
    contrib = mm(solved[...], coupling[...], NT)
    lane = lax.broadcasted_iota(jnp.int32, (1, 128), 1)
    live = lane < count[0, 0]
    contrib = jnp.where(live, contrib, 0.0)
    high = contrib.astype(BF16)
    low = (contrib - high.astype(F32)).astype(BF16)
    both = jnp.concatenate([high, low], axis=0)
    rows = jnp.where(live, sub_map[...], -1)
    batch = contrib.shape[0]
    iota = lax.broadcasted_iota(jnp.int32, (256, 128), 0)
    for block in range(keep.shape[0]):
        hot = jnp.where(iota == rows - block * 256, 1.0, 0.0).astype(BF16)
        spread = mm(both, hot, NT)
        spread = spread[:batch] + spread[batch:]
        first, second = spread[:, :128], spread[:, 128:]
        keep[block] = jnp.where(c == 0, first, second)
        send[block] = jnp.where(c == 0, second, first).astype(BF16)


def forward_kernel(arrived, rhs, slab, keep, send):
    c = lax.axis_index("c")
    total = jnp.sum(arrived[...].astype(F32), axis=0)
    assembled = (rhs[...] - total).astype(BF16)
    for block in range(keep.shape[0]):
        part = mm(assembled, slab[block * 256 : (block + 1) * 256, :], NT)
        first, second = part[:, :128], part[:, 128:]
        keep[block] = jnp.where(c == 0, first, second)
        send[block] = jnp.where(c == 0, second, first).astype(BF16)


def fold_kernel(base, border, columns, out):
    width = 256
    cols = columns[...]
    lane = lax.broadcasted_iota(jnp.int32, (1, 128), 1)
    left = border[...]
    for block in range(out.shape[1] // width):
        start = base + block * width
        halves = [
            jnp.where(cols == lane + (start + half * 128), 1.0, 0.0).astype(BF16)
            for half in range(width // 128)
        ]
        hot = jnp.concatenate(halves, axis=1)
        out[:, block * width : (block + 1) * width] = mm(left, hot).astype(BF16)


def border_kernel(arrived, b0, b1, b2, source, forward, keep, send, b3, sem):
    c = lax.axis_index("c")
    width = keep.shape[2]
    copy = pltpu.make_async_copy(source, b3, sem)
    copy.start()
    total = jnp.sum(arrived[...].astype(F32), axis=0)
    forward[...] = total
    half = total.astype(BF16)
    for x, folded in enumerate((b0, b1, b2, b3)):
        if x == 3:
            copy.wait()
        for y in range(4):
            part = mm(half, folded[:, y * width : (y + 1) * width])
            first, second = part[:16], part[16:]
            keep[y * 4 + x] = jnp.where(c == 0, first, second)
            send[y * 4 + x] = jnp.where(c == 0, second, first).astype(BF16)


def load_kernel(*refs):
    n = len(refs) // 3
    copies = [pltpu.make_async_copy(*each) for each in zip(refs[:n], refs[n : 2 * n], refs[2 * n :])]
    for copy in copies:
        copy.start()
    for copy in copies:
        copy.wait()


def loaded_beside(first, last, arrays, name):
    first, *arrays = lax.optimization_barrier((first, *arrays))
    other = last(first)
    outs = [pltpu.VMEM(a.shape, a.dtype) for a in arrays]
    near = pl.pallas_call(
        load_kernel,
        out_shape=outs,
        in_specs=[pl.BlockSpec(memory_space=pl.ANY)] * len(arrays),
        out_specs=[vmem()] * len(arrays),
        scratch_shapes=[pltpu.SemaphoreType.DMA] * len(arrays),
        cost_estimate=pl.CostEstimate(flops=1 << 30, bytes_accessed=1 << 22, transcendentals=0),
        name=name,
    )(*arrays)
    return first, *lax.optimization_barrier((other, *near))


def pick(index, items):
    out = items[0]
    for k, item in enumerate(items[1:], 1):
        out = jnp.where(index == k, item, out)
    return out


def root_forward_kernel(whole, inverse, out):
    width = whole.shape[2]
    total = None
    for y in range(4):
        left = jnp.concatenate([whole[2 * y], whole[2 * y + 1]], axis=0)
        part = mm(left, inverse[:, y * width : (y + 1) * width], NT)
        total = part if total is None else total + part
    out[...] = total


def root_back_kernel(p0, p1, p2, p3, inverse, forward, out):
    x = lax.axis_index("x")
    parts = (p0[...], p1[...], p2[...], p3[...])
    total = None
    for panel in range(4):
        part = pick(lax.rem(x - panel + 4, 4), parts)
        total = part if total is None else total + part
    forward[...] = total
    half = total.astype(BF16)
    width = out.shape[2]
    for y in range(4):
        part = mm(half, inverse[:, y * width : (y + 1) * width]).astype(BF16)
        out[2 * y] = part[:16]
        out[2 * y + 1] = part[16:]


def residual_kernel(own, other, forward, b0, b1, s2, s3, residual, far, b2, b3, solution, d2, d3, d4):
    c, x_at = lax.axis_index("c"), lax.axis_index("x")
    width = own.shape[2]
    copies = [pltpu.make_async_copy(s2, b2, d2), pltpu.make_async_copy(s3, b3, d3)]
    for copy in copies:
        copy.start()
    for y in range(4):
        first, second = first_second(c, own[y * 4 + x_at], other[y * 4 + x_at])
        cols = slice(y * width, (y + 1) * width)
        solution[:16, cols] = first.astype(F32)
        solution[16:, cols] = second.astype(F32)
    out_copy = pltpu.make_async_copy(solution, far, d4)
    out_copy.start()
    total = None
    for x, folded in enumerate((b0, b1, b2, b3)):
        if x >= 2:
            copies[x - 2].wait()
        for y in range(4):
            left = jnp.concatenate(first_second(c, own[y * 4 + x], other[y * 4 + x]), axis=0)
            part = mm(left, folded[:, y * width : (y + 1) * width], NT)
            total = part if total is None else total + part
    residual[...] = (forward[...] - total).astype(BF16)
    out_copy.wait()


def front_kernel(own, other, slab, out, half):
    c = lax.axis_index("c")
    total = None
    for block in range(own.shape[0]):
        left = jnp.concatenate(first_second(c, own[block], other[block]), axis=1)
        part = mm(left, slab[block * 256 : (block + 1) * 256, :])
        total = part if total is None else total + part
    out[:, 0, :] = total
    half[...] = total.astype(BF16)


def update_kernel(count, own, other, sub_map, coupling, out):
    c = lax.axis_index("c")
    lane = lax.broadcasted_iota(jnp.int32, (1, 128), 1)
    rows = jnp.where(lane < count[0, 0], sub_map[...], -1)
    iota = lax.broadcasted_iota(jnp.int32, (256, 128), 0)
    total = None
    for block in range(own.shape[0]):
        left = jnp.concatenate(first_second(c, own[block], other[block]), axis=1)
        hot = jnp.where(iota == rows - block * 256, 1.0, 0.0).astype(BF16)
        part = mm(left, hot)
        total = part if total is None else total + part
    out[:, 0, :] = mm(total.astype(BF16), coupling[...])


def swap_core(x):
    return lax.ppermute(x, "c", [(0, 1), (1, 0)])


def shifted(x, axis, k):
    return lax.ppermute(x, axis, [(i, (i + k) % 4) for i in range(4)])


def exchange(x, axes):
    return lax.all_to_all(x, axes, split_axis=0, concat_axis=0, tiled=True)


def to_everyone(x, axes, peers):
    return exchange(jnp.broadcast_to(x, (peers, *x.shape)), axes)


def joined(keep, got):
    return keep + got.astype(F32)


def body(
    subtree_solution,
    subtree_coupling,
    sub_map,
    sub_count,
    front_rhs,
    sep_inverse,
    border_coupling,
    border_map,
    root_rhs,
    root_inverse,
):
    z_size, y_size = lax.axis_size("z"), lax.axis_size("y")
    peers = z_size * y_size
    c, y, x = lax.axis_index("c"), lax.axis_index("y"), lax.axis_index("x")
    solved = subtree_solution[:, 0, :]
    coupling = subtree_coupling[0]
    slab = sep_inverse[0]
    border = border_coupling[0]
    batch = solved.shape[0]
    split = like((peers, batch, 128), F32), like((peers, batch, 128), BF16)

    own_map = lax.dynamic_index_in_dim(border_map, x, 0, keepdims=False)
    columns = jnp.broadcast_to(own_map[:, None], (own_map.shape[0], 128))
    panel_width = root_rhs.shape[1]
    folded = []
    for panel in range(4):
        call = kernel_call(
            lambda b, k, o, base=panel * panel_width: fold_kernel(base, b, k, o),
            like((border.shape[0], panel_width), BF16),
            0,
            2,
            flops=2 * border.shape[0] * border.shape[1] * panel_width,
            name=f"fold{panel}",
        )
        folded.append(call(border, columns))

    keep, send = kernel_call(scatter_kernel, split, 1, 3, name="scatter", near_out=(0, 1))(
        sub_count, solved, coupling, sub_map
    )
    arrived = exchange(joined(keep, swap_core(send)).astype(BF16), ("z", "y"))
    arrived, *folded[:2] = lax.optimization_barrier((arrived, *folded[:2]))
    keep, send = kernel_call(
        forward_kernel,
        split,
        0,
        3,
        name="forward",
        near=(0, 2),
        near_out=(0, 1),
    )(arrived, front_rhs[:, 0, :], slab)
    arrived = exchange(joined(keep, swap_core(send)).astype(BF16), ("z", "y"))

    quarter = panel_width // 4
    forward, keep, send = kernel_call(
        border_kernel,
        (like((batch, 128), F32), like((16, 16, quarter), F32), like((16, 16, quarter), BF16)),
        0,
        4,
        name="border",
        near=(0, 1, 2, 3),
        near_out=(0, 1, 2),
        stream=[folded[3].shape],
    )(arrived, *folded)
    rhs_part = lax.dynamic_slice(root_rhs, (c * 16, y * quarter), (16, quarter))
    joint = joined(keep, swap_core(send)).astype(BF16)
    joint, rhs_part = lax.optimization_barrier((joint, rhs_part))
    arrived = exchange(joint, ("y", "x"))
    near = arrived.astype(F32).sum(axis=0).astype(BF16)
    border_sum = to_everyone(near, "z", z_size).astype(F32).sum(axis=0)
    chunk = (rhs_part - border_sum).astype(BF16)
    whole = to_everyone(chunk, ("y", "c"), 8)
    partial = kernel_call(
        root_forward_kernel,
        like((batch, root_inverse.shape[0]), F32),
        0,
        2,
        name="rootf",
        near=(0, 1),
        near_out=(0,),
    )(whole, root_inverse)

    parts = [partial] + [shifted(partial, "x", k) for k in (1, 2, 3)]
    root_forward, col = kernel_call(
        root_back_kernel,
        (like((batch, root_inverse.shape[0]), F32), like((8, 16, quarter), BF16)),
        0,
        5,
        name="rootb",
        near=(0, 1, 2, 3, 4),
        near_out=(1,),
    )(*parts, root_inverse)
    near = exchange(col, ("y", "c")).astype(F32).sum(axis=0).astype(BF16)
    chunk = to_everyone(near, "z", z_size).astype(F32).sum(axis=0).astype(BF16)
    own = to_everyone(chunk, ("y", "x"), 16)
    own, other, *near_folds = loaded_beside(own, swap_core, folded[:2], "loadfold")
    residual, root_solution = kernel_call(
        residual_kernel,
        (like((batch, 128), BF16), like((batch, panel_width), F32)),
        0,
        5,
        name="resid",
        near=(0, 1, 2, 3, 4),
        near_out=(0,),
        stream=[f.shape for f in folded[2:]],
        far_out=(1,),
    )(own, other, forward, *near_folds, *folded[2:])

    own = to_everyone(residual, ("z", "y"), peers)
    own, other, near_slab = loaded_beside(own, swap_core, [slab], "loadslab")
    front_solution, front_half = kernel_call(
        front_kernel,
        (like((batch, 1, 128), F32), like((batch, 128), BF16)),
        0,
        3,
        name="front",
        near=(0, 1, 2),
        near_out=(0, 1),
    )(own, other, near_slab)
    front_half, coupling = lax.optimization_barrier((front_half, coupling))
    own = to_everyone(front_half, ("z", "y"), peers)
    subtree_update = kernel_call(
        update_kernel,
        like((batch, 1, coupling.shape[1]), F32),
        1,
        4,
        name="update",
        near=(0, 1, 3),
    )(sub_count, own, swap_core(own), sub_map, coupling)
    return (root_forward, root_solution, front_solution, subtree_update)


def solution(mesh):
    finer = Mesh(mesh.devices.reshape(8, 4, 2, mesh.shape["panel"]), ("z", "y", "c", "x"))
    in_specs = (
        P(None, "x", LEAF),
        P("x", LEAF, None),
        P("x", LEAF),
        P("x", LEAF),
        P(None, "x", LEAF),
        P("x", None, LEAF),
        P("x", LEAF, None),
        P(None, None),
        P(None, "x"),
        P(LEAF, "x"),
    )
    out_specs = (P(None, LEAF), P(None, "x"), P(None, "x", LEAF), P(None, "x", LEAF))
    return jax.shard_map(
        body, mesh=finer, in_specs=in_specs, out_specs=out_specs, check_vma=False
    )
```

```python
import jax
import jax.numpy as jnp
from jax import lax
from jax.experimental import pallas as pl
from jax.experimental.pallas import tpu as pltpu
from jax.sharding import Mesh
from jax.sharding import PartitionSpec as P

LEAF = ("z", "y", "c")
F32, BF16 = jnp.float32, jnp.bfloat16
NT = (((1,), (1,)), ((), ()))
NN = (((1,), (0,)), ((), ()))


def mm(a, b, dims=NN):
    return lax.dot_general(a, b, dims, preferred_element_type=F32)


def smem():
    return pl.BlockSpec(memory_space=pltpu.SMEM)


def vmem():
    return pl.BlockSpec(memory_space=pltpu.VMEM)


def kernel_call(body, outs, n_smem, n_vmem, flops=0, name=None, near=(), near_out=(), stream=(), far_out=()):
    flat, tree = jax.tree.flatten(outs)
    flat = [pltpu.VMEM(o.shape, o.dtype) if i in near_out else o for i, o in enumerate(flat)]
    call = pl.pallas_call(
        body,
        out_shape=jax.tree.unflatten(tree, flat),
        in_specs=[smem()] * n_smem
        + [vmem()] * n_vmem
        + [pl.BlockSpec(memory_space=pl.ANY)] * len(stream),
        out_specs=jax.tree.unflatten(
            tree,
            [pl.BlockSpec(memory_space=pl.ANY) if i in far_out else vmem() for i in range(len(flat))],
        ),
        scratch_shapes=[pltpu.VMEM(x, BF16) for x in stream]
        + [pltpu.VMEM(flat[i].shape, flat[i].dtype) for i in far_out]
        + [pltpu.SemaphoreType.DMA] * (2 * len(stream) + len(far_out)),
        cost_estimate=pl.CostEstimate(flops=flops, bytes_accessed=flops // 64, transcendentals=0) if flops else None,
        name=name,
    )

    def run(*args):
        args = list(args)
        for i in near:
            args[n_smem + i] = pltpu.with_memory_space_constraint(args[n_smem + i], pltpu.VMEM)
        return call(*args)

    return run


def like(shape, dtype):
    return jax.ShapeDtypeStruct(shape, dtype)


def first_second(c, mine, theirs):
    return jnp.where(c == 0, mine, theirs), jnp.where(c == 0, theirs, mine)


def scatter_kernel(count, solved, coupling, sub_map, keep, send, live_rows):
    c = lax.axis_index("c")
    contrib = mm(solved[...], coupling[...], NT)
    lane = lax.broadcasted_iota(jnp.int32, (1, 128), 1)
    live = lane < count[0, 0]
    contrib = jnp.where(live, contrib, 0.0)
    high = contrib.astype(BF16)
    low = (contrib - high.astype(F32)).astype(BF16)
    both = jnp.concatenate([high, low], axis=0)
    rows = jnp.where(live, sub_map[...], -1)
    live_rows[...] = rows
    batch = contrib.shape[0]
    iota = lax.broadcasted_iota(jnp.int32, (256, 128), 0)
    for block in range(keep.shape[0]):
        hot = jnp.where(iota == rows - block * 256, 1.0, 0.0).astype(BF16)
        spread = mm(both, hot, NT)
        spread = spread[:batch] + spread[batch:]
        first, second = spread[:, :128], spread[:, 128:]
        keep[block] = jnp.where(c == 0, first, second)
        send[block] = jnp.where(c == 0, second, first).astype(BF16)


def forward_kernel(arrived, rhs, slab, keep, send):
    c = lax.axis_index("c")
    total = jnp.sum(arrived[...].astype(F32), axis=0)
    assembled = (rhs[...] - total).astype(BF16)
    for block in range(keep.shape[0]):
        part = mm(assembled, slab[block * 256 : (block + 1) * 256, :], NT)
        first, second = part[:, :128], part[:, 128:]
        keep[block] = jnp.where(c == 0, first, second)
        send[block] = jnp.where(c == 0, second, first).astype(BF16)


def fold_kernel(base, border, columns, out):
    width = 256
    cols = columns[...]
    lane = lax.broadcasted_iota(jnp.int32, (1, 128), 1)
    left = border[...]
    for block in range(out.shape[1] // width):
        start = base + block * width
        halves = [
            jnp.where(cols == lane + (start + half * 128), 1.0, 0.0).astype(BF16)
            for half in range(width // 128)
        ]
        hot = jnp.concatenate(halves, axis=1)
        out[:, block * width : (block + 1) * width] = mm(left, hot).astype(BF16)


def half_copies(source, buffer, sems):
    width = source.shape[1] // 2
    return [
        pltpu.make_async_copy(
            source.at[:, pl.ds(i * width, width)], buffer.at[:, pl.ds(i * width, width)], sem
        )
        for i, sem in enumerate(sems)
    ]


def border_kernel(arrived, early, source, forward, keep, send, late, *sems):
    c = lax.axis_index("c")
    width = keep.shape[2]
    copies = half_copies(source, late, sems)
    for copy in copies:
        copy.start()
    total = jnp.sum(arrived[...].astype(F32), axis=0)
    forward[...] = total
    half = total.astype(BF16)
    for x in range(4):
        if x >= 2:
            copies[x - 2].wait()
        for y in range(4):
            at = (x % 2 * 4 + y) * width
            part = mm(half, (early, late)[x // 2][:, at : at + width])
            first, second = part[:16], part[16:]
            keep[y * 4 + x] = jnp.where(c == 0, first, second)
            send[y * 4 + x] = jnp.where(c == 0, second, first).astype(BF16)


def load_kernel(*refs):
    n = len(refs) // 3
    copies = [pltpu.make_async_copy(*each) for each in zip(refs[:n], refs[n : 2 * n], refs[2 * n :])]
    for copy in copies:
        copy.start()
    for copy in copies:
        copy.wait()


def loaded_beside(first, last, arrays, name):
    first, *arrays = lax.optimization_barrier((first, *arrays))
    other = last(first)
    outs = [pltpu.VMEM(a.shape, a.dtype) for a in arrays]
    near = pl.pallas_call(
        load_kernel,
        out_shape=outs,
        in_specs=[pl.BlockSpec(memory_space=pl.ANY)] * len(arrays),
        out_specs=[vmem()] * len(arrays),
        scratch_shapes=[pltpu.SemaphoreType.DMA] * len(arrays),
        cost_estimate=pl.CostEstimate(flops=1 << 30, bytes_accessed=1 << 22, transcendentals=0),
        name=name,
    )(*arrays)
    return first, *lax.optimization_barrier((other, *near))


def pick(index, items):
    out = items[0]
    for k, item in enumerate(items[1:], 1):
        out = jnp.where(index == k, item, out)
    return out


def root_forward_kernel(whole, inverse, out):
    width = whole.shape[2]
    total = None
    for y in range(4):
        left = jnp.concatenate([whole[2 * y], whole[2 * y + 1]], axis=0)
        part = mm(left, inverse[:, y * width : (y + 1) * width], NT)
        total = part if total is None else total + part
    out[...] = total


def root_back_kernel(p0, p1, p2, p3, inverse, far, out, forward, sem):
    x = lax.axis_index("x")
    parts = (p0[...], p1[...], p2[...], p3[...])
    total = None
    for panel in range(4):
        part = pick(lax.rem(x - panel + 4, 4), parts)
        total = part if total is None else total + part
    forward[...] = total
    copy = pltpu.make_async_copy(forward, far, sem)
    copy.start()
    half = total.astype(BF16)
    width = out.shape[2]
    for y in range(4):
        part = mm(half, inverse[:, y * width : (y + 1) * width]).astype(BF16)
        out[2 * y] = part[:16]
        out[2 * y + 1] = part[16:]
    copy.wait()


def residual_kernel(own, other, forward, early, source, residual, far, late, solution, *sems):
    c, x_at = lax.axis_index("c"), lax.axis_index("x")
    width = own.shape[2]
    copies = half_copies(source, late, sems[:2])
    for copy in copies:
        copy.start()
    for y in range(4):
        first, second = first_second(c, own[y * 4 + x_at], other[y * 4 + x_at])
        cols = slice(y * width, (y + 1) * width)
        solution[:16, cols] = first.astype(F32)
        solution[16:, cols] = second.astype(F32)
    out_copy = pltpu.make_async_copy(solution, far, sems[2])
    out_copy.start()
    total = None
    for x in range(4):
        if x >= 2:
            copies[x - 2].wait()
        for y in range(4):
            left = jnp.concatenate(first_second(c, own[y * 4 + x], other[y * 4 + x]), axis=0)
            at = (x % 2 * 4 + y) * width
            part = mm(left, (early, late)[x // 2][:, at : at + width], NT)
            total = part if total is None else total + part
    residual[...] = (forward[...] - total).astype(BF16)
    out_copy.wait()


def front_kernel(own, other, slab, out, half):
    c = lax.axis_index("c")
    total = None
    for block in range(own.shape[0]):
        left = jnp.concatenate(first_second(c, own[block], other[block]), axis=1)
        part = mm(left, slab[block * 256 : (block + 1) * 256, :])
        total = part if total is None else total + part
    out[:, 0, :] = total
    half[...] = total.astype(BF16)


def update_kernel(own, other, live_rows, coupling, out):
    c = lax.axis_index("c")
    rows = live_rows[...]
    iota = lax.broadcasted_iota(jnp.int32, (256, 128), 0)
    total = None
    for block in range(own.shape[0]):
        left = jnp.concatenate(first_second(c, own[block], other[block]), axis=1)
        hot = jnp.where(iota == rows - block * 256, 1.0, 0.0).astype(BF16)
        part = mm(left, hot)
        total = part if total is None else total + part
    out[:, 0, :] = mm(total.astype(BF16), coupling[...])


def swap_core(x):
    return lax.ppermute(x, "c", [(0, 1), (1, 0)])


def shifted(x, axis, k):
    return lax.ppermute(x, axis, [(i, (i + k) % 4) for i in range(4)])


def exchange(x, axes):
    return lax.all_to_all(x, axes, split_axis=0, concat_axis=0, tiled=True)


def to_everyone(x, axes, peers):
    return exchange(jnp.broadcast_to(x, (peers, *x.shape)), axes)


def joined(keep, got):
    return keep + got.astype(F32)


def body(
    subtree_solution,
    subtree_coupling,
    sub_map,
    sub_count,
    front_rhs,
    sep_inverse,
    border_coupling,
    border_map,
    root_rhs,
    root_inverse,
):
    z_size, y_size = lax.axis_size("z"), lax.axis_size("y")
    peers = z_size * y_size
    c, y, x = lax.axis_index("c"), lax.axis_index("y"), lax.axis_index("x")
    solved = subtree_solution[:, 0, :]
    coupling = subtree_coupling[0]
    slab = sep_inverse[0]
    border = border_coupling[0]
    batch = solved.shape[0]
    split = like((peers, batch, 128), F32), like((peers, batch, 128), BF16)

    own_map = lax.dynamic_index_in_dim(border_map, x, 0, keepdims=False)
    columns = jnp.broadcast_to(own_map[:, None], (own_map.shape[0], 128))
    panel_width = root_rhs.shape[1]
    folded = []
    for pair in range(2):
        call = kernel_call(
            lambda b, k, o, base=pair * 2 * panel_width: fold_kernel(base, b, k, o),
            like((border.shape[0], 2 * panel_width), BF16),
            0,
            2,
            flops=4 * border.shape[0] * border.shape[1] * panel_width,
            name=f"fold{pair}",
        )
        folded.append(call(border, columns))

    keep, send, live_rows = kernel_call(
        scatter_kernel,
        (*split, like(sub_map.shape, jnp.int32)),
        1,
        3,
        name="scatter",
        near_out=(0, 1, 2),
    )(sub_count, solved, coupling, sub_map)
    arrived = exchange(joined(keep, swap_core(send)).astype(BF16), ("z", "y"))
    arrived, folded[0] = lax.optimization_barrier((arrived, folded[0]))
    keep, send = kernel_call(
        forward_kernel,
        split,
        0,
        3,
        name="forward",
        near=(0, 1, 2),
        near_out=(0, 1),
    )(arrived, front_rhs[:, 0, :], slab)
    arrived = exchange(joined(keep, swap_core(send)).astype(BF16), ("z", "y"))

    quarter = panel_width // 4
    forward, keep, send = kernel_call(
        border_kernel,
        (like((batch, 128), F32), like((16, 16, quarter), F32), like((16, 16, quarter), BF16)),
        0,
        2,
        name="border",
        near=(0, 1),
        near_out=(0, 1, 2),
        stream=[folded[1].shape],
    )(arrived, *folded)
    rhs_part = lax.dynamic_slice(root_rhs, (c * 16, y * quarter), (16, quarter))
    joint = joined(keep, swap_core(send)).astype(BF16)
    joint, rhs_part = lax.optimization_barrier((joint, rhs_part))
    arrived = exchange(joint, ("y", "x"))
    near = arrived.astype(F32).sum(axis=0).astype(BF16)
    border_sum = to_everyone(near, "z", z_size).astype(F32).sum(axis=0)
    chunk = (rhs_part - border_sum).astype(BF16)
    whole = to_everyone(chunk, ("y", "c"), 8)
    partial = kernel_call(
        root_forward_kernel,
        like((batch, root_inverse.shape[0]), F32),
        0,
        2,
        name="rootf",
        near=(0, 1),
        near_out=(0,),
    )(whole, root_inverse)

    parts = [partial] + [shifted(partial, "x", k) for k in (1, 2, 3)]
    root_forward, col = kernel_call(
        root_back_kernel,
        (like((batch, root_inverse.shape[0]), F32), like((8, 16, quarter), BF16)),
        0,
        5,
        name="rootb",
        near=(0, 1, 2, 3, 4),
        near_out=(1,),
        far_out=(0,),
    )(*parts, root_inverse)
    near = exchange(col, ("y", "c")).astype(F32).sum(axis=0).astype(BF16)
    chunk = to_everyone(near, "z", z_size).astype(F32).sum(axis=0).astype(BF16)
    own = to_everyone(chunk, ("y", "x"), 16)
    own, other, near_fold = loaded_beside(own, swap_core, folded[:1], "loadfold")
    residual, root_solution = kernel_call(
        residual_kernel,
        (like((batch, 128), BF16), like((batch, panel_width), F32)),
        0,
        4,
        name="resid",
        near=(0, 1, 2, 3),
        near_out=(0,),
        stream=[folded[1].shape],
        far_out=(1,),
    )(own, other, forward, near_fold, folded[1])

    own = to_everyone(residual, ("z", "y"), peers)
    own, other, near_slab = loaded_beside(own, swap_core, [slab], "loadslab")
    front_solution, front_half = kernel_call(
        front_kernel,
        (like((batch, 1, 128), F32), like((batch, 128), BF16)),
        0,
        3,
        name="front",
        near=(0, 1, 2),
        near_out=(0, 1),
    )(own, other, near_slab)
    own = to_everyone(front_half, ("z", "y"), peers)
    own, other, near_coupling = loaded_beside(own, swap_core, [coupling], "loadcoup")
    subtree_update = kernel_call(
        update_kernel,
        like((batch, 1, coupling.shape[1]), F32),
        0,
        4,
        name="update",
        near=(0, 1, 2, 3),
    )(own, other, live_rows, near_coupling)
    return (root_forward, root_solution, front_solution, subtree_update)


def solution(mesh):
    finer = Mesh(mesh.devices.reshape(8, 4, 2, mesh.shape["panel"]), ("z", "y", "c", "x"))
    in_specs = (
        P(None, "x", LEAF),
        P("x", LEAF, None),
        P("x", LEAF),
        P("x", LEAF),
        P(None, "x", LEAF),
        P("x", None, LEAF),
        P("x", LEAF, None),
        P(None, None),
        P(None, "x"),
        P(LEAF, "x"),
    )
    out_specs = (P(None, LEAF), P(None, "x"), P(None, "x", LEAF), P(None, "x", LEAF))
    return jax.shard_map(
        body, mesh=finer, in_specs=in_specs, out_specs=out_specs, check_vma=False
    )
```

```python
import jax
import jax.numpy as jnp
from jax import lax
from jax.experimental import pallas as pl
from jax.experimental.pallas import tpu as pltpu
from jax.sharding import Mesh
from jax.sharding import PartitionSpec as P

LEAF = ("z", "y", "c")
F32, BF16 = jnp.float32, jnp.bfloat16
NT = (((1,), (1,)), ((), ()))
NN = (((1,), (0,)), ((), ()))


def mm(a, b, dims=NN):
    return lax.dot_general(a, b, dims, preferred_element_type=F32)


def smem():
    return pl.BlockSpec(memory_space=pltpu.SMEM)


def vmem():
    return pl.BlockSpec(memory_space=pltpu.VMEM)


def kernel_call(body, outs, n_smem, n_vmem, flops=0, name=None, near=(), near_out=(), stream=(), far_out=()):
    flat, tree = jax.tree.flatten(outs)
    flat = [pltpu.VMEM(o.shape, o.dtype) if i in near_out else o for i, o in enumerate(flat)]
    call = pl.pallas_call(
        body,
        out_shape=jax.tree.unflatten(tree, flat),
        in_specs=[smem()] * n_smem
        + [vmem()] * n_vmem
        + [pl.BlockSpec(memory_space=pl.ANY)] * len(stream),
        out_specs=jax.tree.unflatten(
            tree,
            [pl.BlockSpec(memory_space=pl.ANY) if i in far_out else vmem() for i in range(len(flat))],
        ),
        scratch_shapes=[pltpu.VMEM(x, BF16) for x in stream]
        + [pltpu.VMEM(flat[i].shape, flat[i].dtype) for i in far_out]
        + [pltpu.SemaphoreType.DMA] * (2 * len(stream) + len(far_out)),
        cost_estimate=pl.CostEstimate(flops=flops, bytes_accessed=flops // 64, transcendentals=0) if flops else None,
        name=name,
    )

    def run(*args):
        args = list(args)
        for i in near:
            args[n_smem + i] = pltpu.with_memory_space_constraint(args[n_smem + i], pltpu.VMEM)
        return call(*args)

    return run


def like(shape, dtype):
    return jax.ShapeDtypeStruct(shape, dtype)


def first_second(c, mine, theirs):
    return jnp.where(c == 0, mine, theirs), jnp.where(c == 0, theirs, mine)


def scatter_kernel(count, solved, coupling, sub_map, keep, send, live_rows):
    c = lax.axis_index("c")
    contrib = mm(solved[...], coupling[...], NT)
    lane = lax.broadcasted_iota(jnp.int32, (1, 128), 1)
    live = lane < count[0, 0]
    contrib = jnp.where(live, contrib, 0.0)
    high = contrib.astype(BF16)
    low = (contrib - high.astype(F32)).astype(BF16)
    both = jnp.concatenate([high, low], axis=0)
    rows = jnp.where(live, sub_map[...], -1)
    live_rows[...] = rows
    batch = contrib.shape[0]
    iota = lax.broadcasted_iota(jnp.int32, (256, 128), 0)
    for block in range(keep.shape[0]):
        hot = jnp.where(iota == rows - block * 256, 1.0, 0.0).astype(BF16)
        spread = mm(both, hot, NT)
        spread = spread[:batch] + spread[batch:]
        first, second = spread[:, :128], spread[:, 128:]
        keep[block] = jnp.where(c == 0, first, second)
        send[block] = jnp.where(c == 0, second, first).astype(BF16)


def forward_kernel(arrived, rhs, slab, keep, send):
    c = lax.axis_index("c")
    total = jnp.sum(arrived[...].astype(F32), axis=0)
    assembled = (rhs[...] - total).astype(BF16)
    for block in range(keep.shape[0]):
        part = mm(assembled, slab[block * 256 : (block + 1) * 256, :], NT)
        first, second = part[:, :128], part[:, 128:]
        keep[block] = jnp.where(c == 0, first, second)
        send[block] = jnp.where(c == 0, second, first).astype(BF16)


def fold_kernel(base, border, columns, out):
    width = 256
    cols = columns[...]
    lane = lax.broadcasted_iota(jnp.int32, (1, 128), 1)
    left = border[...]
    for block in range(out.shape[1] // width):
        start = base + block * width
        halves = [
            jnp.where(cols == lane + (start + half * 128), 1.0, 0.0).astype(BF16)
            for half in range(width // 128)
        ]
        hot = jnp.concatenate(halves, axis=1)
        out[:, block * width : (block + 1) * width] = mm(left, hot).astype(BF16)


def half_copies(source, buffer, sems):
    width = source.shape[1] // 2
    return [
        pltpu.make_async_copy(
            source.at[:, pl.ds(i * width, width)], buffer.at[:, pl.ds(i * width, width)], sem
        )
        for i, sem in enumerate(sems)
    ]


def border_kernel(arrived, early, source, forward, keep, send, late, *sems):
    c = lax.axis_index("c")
    width = keep.shape[2]
    copies = half_copies(source, late, sems)
    for copy in copies:
        copy.start()
    total = jnp.sum(arrived[...].astype(F32), axis=0)
    forward[...] = total
    half = total.astype(BF16)
    for x in range(4):
        if x >= 2:
            copies[x - 2].wait()
        for y in range(4):
            at = (x % 2 * 4 + y) * width
            part = mm(half, (early, late)[x // 2][:, at : at + width])
            first, second = part[:16], part[16:]
            keep[y * 4 + x] = jnp.where(c == 0, first, second).astype(BF16)
            send[y * 4 + x] = jnp.where(c == 0, second, first).astype(BF16)


def load_kernel(*refs):
    n = len(refs) // 3
    copies = [pltpu.make_async_copy(*each) for each in zip(refs[:n], refs[n : 2 * n], refs[2 * n :])]
    for copy in copies:
        copy.start()
    for copy in copies:
        copy.wait()


def loaded_beside(first, last, arrays, name):
    first, *arrays = lax.optimization_barrier((first, *arrays))
    other = last(first)
    outs = [pltpu.VMEM(a.shape, a.dtype) for a in arrays]
    near = pl.pallas_call(
        load_kernel,
        out_shape=outs,
        in_specs=[pl.BlockSpec(memory_space=pl.ANY)] * len(arrays),
        out_specs=[vmem()] * len(arrays),
        scratch_shapes=[pltpu.SemaphoreType.DMA] * len(arrays),
        cost_estimate=pl.CostEstimate(flops=1 << 30, bytes_accessed=1 << 22, transcendentals=0),
        name=name,
    )(*arrays)
    return first, *lax.optimization_barrier((other, *near))


def pick(index, items):
    out = items[0]
    for k, item in enumerate(items[1:], 1):
        out = jnp.where(index == k, item, out)
    return out


def root_forward_kernel(whole, mine, theirs, out):
    width = whole.shape[2]
    for k, inverse in enumerate((mine, theirs)):
        total = None
        for y in range(4):
            part = mm(whole[y], inverse[:, y * width : (y + 1) * width], NT)
            total = part if total is None else total + part
        out[k] = total


def root_back_kernel(p0, p1, p2, p3, mine, theirs, forward, out):
    x = lax.axis_index("x")
    parts = (p0[...], p1[...], p2[...], p3[...])
    total = None
    for panel in range(4):
        part = pick(lax.rem(x - panel + 4, 4), parts)
        total = part if total is None else total + part
    forward[...] = total
    half = total.astype(BF16)
    width = out.shape[2]
    for y in range(4):
        cols = slice(y * width, (y + 1) * width)
        out[y] = (mm(half[0], mine[:, cols]) + mm(half[1], theirs[:, cols])).astype(BF16)


def residual_kernel(own, other, forward, early, source, residual, far, late, solution, *sems):
    c, x_at = lax.axis_index("c"), lax.axis_index("x")
    width = own.shape[2]
    copies = half_copies(source, late, sems[:2])
    for copy in copies:
        copy.start()
    for y in range(4):
        first, second = first_second(c, own[y * 4 + x_at], other[y * 4 + x_at])
        cols = slice(y * width, (y + 1) * width)
        solution[:16, cols] = first.astype(F32)
        solution[16:, cols] = second.astype(F32)
    out_copy = pltpu.make_async_copy(solution, far, sems[2])
    out_copy.start()
    total = None
    for x in range(4):
        if x >= 2:
            copies[x - 2].wait()
        for y in range(4):
            left = jnp.concatenate(first_second(c, own[y * 4 + x], other[y * 4 + x]), axis=0)
            at = (x % 2 * 4 + y) * width
            part = mm(left, (early, late)[x // 2][:, at : at + width], NT)
            total = part if total is None else total + part
    residual[...] = (forward[...] - total).astype(BF16)
    out_copy.wait()


def front_kernel(own, other, slab, ours, later, far, out, half, forward, sem):
    c = lax.axis_index("c")
    first, second = first_second(c, ours[0], later[...])
    forward[:16, :] = first
    forward[16:, :] = second
    copy = pltpu.make_async_copy(forward, far, sem)
    copy.start()
    total = None
    for block in range(own.shape[0]):
        left = jnp.concatenate(first_second(c, own[block], other[block]), axis=1)
        part = mm(left, slab[block * 256 : (block + 1) * 256, :])
        total = part if total is None else total + part
    out[:, 0, :] = total
    half[...] = total.astype(BF16)
    copy.wait()


def update_kernel(own, other, live_rows, coupling, out):
    c = lax.axis_index("c")
    rows = live_rows[...]
    iota = lax.broadcasted_iota(jnp.int32, (256, 128), 0)
    total = None
    for block in range(own.shape[0]):
        left = jnp.concatenate(first_second(c, own[block], other[block]), axis=1)
        hot = jnp.where(iota == rows - block * 256, 1.0, 0.0).astype(BF16)
        part = mm(left, hot)
        total = part if total is None else total + part
    out[:, 0, :] = mm(total.astype(BF16), coupling[...])


def swap_core(x):
    return lax.ppermute(x, "c", [(0, 1), (1, 0)])


def shifted(x, axis, k):
    return lax.ppermute(x, axis, [(i, (i + k) % 4) for i in range(4)])


def exchange(x, axes):
    return lax.all_to_all(x, axes, split_axis=0, concat_axis=0, tiled=True)


def to_everyone(x, axes, peers):
    return exchange(jnp.broadcast_to(x, (peers, *x.shape)), axes)


def joined(keep, got):
    return keep.astype(F32) + got.astype(F32)


def body(
    subtree_solution,
    subtree_coupling,
    sub_map,
    sub_count,
    front_rhs,
    sep_inverse,
    border_coupling,
    border_map,
    root_rhs,
    root_inverse,
):
    z_size, y_size = lax.axis_size("z"), lax.axis_size("y")
    peers = z_size * y_size
    c, y, x = lax.axis_index("c"), lax.axis_index("y"), lax.axis_index("x")
    solved = subtree_solution[:, 0, :]
    coupling = subtree_coupling[0]
    slab = sep_inverse[0]
    border = border_coupling[0]
    batch = solved.shape[0]
    split = like((peers, batch, 128), F32), like((peers, batch, 128), BF16)

    own_map = lax.dynamic_index_in_dim(border_map, x, 0, keepdims=False)
    columns = jnp.broadcast_to(own_map[:, None], (own_map.shape[0], 128))
    panel_width = root_rhs.shape[1]
    folded = []
    for pair in range(2):
        call = kernel_call(
            lambda b, k, o, base=pair * 2 * panel_width: fold_kernel(base, b, k, o),
            like((border.shape[0], 2 * panel_width), BF16),
            0,
            2,
            flops=4 * border.shape[0] * border.shape[1] * panel_width,
            name=f"fold{pair}",
        )
        folded.append(call(border, columns))

    keep, send, live_rows = kernel_call(
        scatter_kernel,
        (*split, like(sub_map.shape, jnp.int32)),
        1,
        3,
        name="scatter",
        near_out=(0, 1, 2),
    )(sub_count, solved, coupling, sub_map)
    arrived = exchange(joined(keep, swap_core(send)).astype(BF16), ("z", "y"))
    arrived, folded[0] = lax.optimization_barrier((arrived, folded[0]))
    keep, send = kernel_call(
        forward_kernel,
        split,
        0,
        3,
        name="forward",
        near=(0, 1, 2),
        near_out=(0, 1),
    )(arrived, front_rhs[:, 0, :], slab)
    joint = joined(keep, swap_core(send)).astype(BF16)
    joint, mine = lax.optimization_barrier((joint, root_inverse))
    theirs = swap_core(mine)
    arrived = exchange(joint, ("z", "y"))
    arrived, mine, theirs = lax.optimization_barrier((arrived, mine, theirs))

    quarter = panel_width // 4
    forward, keep, send = kernel_call(
        border_kernel,
        (like((batch, 128), F32), like((16, 16, quarter), BF16), like((16, 16, quarter), BF16)),
        0,
        2,
        name="border",
        near=(0, 1),
        near_out=(0, 1, 2),
        stream=[folded[1].shape],
    )(arrived, *folded)
    rhs_part = lax.dynamic_slice(root_rhs, (c * 16, y * quarter), (16, quarter))
    joint = joined(keep, swap_core(send)).astype(BF16)
    joint, rhs_part = lax.optimization_barrier((joint, rhs_part))
    arrived = exchange(joint, ("y", "x"))
    near = arrived.astype(F32).sum(axis=0).astype(BF16)
    border_sum = to_everyone(near, "z", z_size).astype(F32).sum(axis=0)
    chunk = (rhs_part - border_sum).astype(BF16)
    whole = to_everyone(chunk, "y", y_size)
    pair = like((2, 16, root_inverse.shape[0]), F32)
    partial = kernel_call(
        root_forward_kernel, pair, 0, 3, name="rootf", near=(0, 1, 2), near_out=(0,)
    )(whole, mine, theirs)

    parts = [partial] + [shifted(partial, "x", k) for k in (1, 2, 3)]
    forward_pair, col = kernel_call(
        root_back_kernel,
        (pair, like((4, 16, quarter), BF16)),
        0,
        6,
        name="rootb",
        near=(0, 1, 2, 3, 4, 5),
        near_out=(0, 1),
    )(*parts, mine, theirs)
    near = exchange(col, "y").astype(F32).sum(axis=0).astype(BF16)
    chunk = to_everyone(near, "z", z_size).astype(F32).sum(axis=0).astype(BF16)
    own = to_everyone(chunk, ("y", "x"), 16)
    own, other, near_fold = loaded_beside(own, swap_core, folded[:1], "loadfold")
    residual, root_solution = kernel_call(
        residual_kernel,
        (like((batch, 128), BF16), like((batch, panel_width), F32)),
        0,
        4,
        name="resid",
        near=(0, 1, 2, 3),
        near_out=(0,),
        stream=[folded[1].shape],
        far_out=(1,),
    )(own, other, forward, near_fold, folded[1])

    own = to_everyone(residual, ("z", "y"), peers)
    own, forward_pair = lax.optimization_barrier((own, forward_pair))
    later = swap_core(forward_pair[1])
    own, other, near_slab = loaded_beside(own, swap_core, [slab], "loadslab")
    root_forward, front_solution, front_half = kernel_call(
        front_kernel,
        (
            like((batch, root_inverse.shape[0]), F32),
            like((batch, 1, 128), F32),
            like((batch, 128), BF16),
        ),
        0,
        5,
        name="front",
        near=(0, 1, 2, 3, 4),
        near_out=(1, 2),
        far_out=(0,),
    )(own, other, near_slab, forward_pair, later)
    own = to_everyone(front_half, ("z", "y"), peers)
    own, other, near_coupling = loaded_beside(own, swap_core, [coupling], "loadcoup")
    subtree_update = kernel_call(
        update_kernel,
        like((batch, 1, coupling.shape[1]), F32),
        0,
        4,
        name="update",
        near=(0, 1, 2, 3),
    )(own, other, live_rows, near_coupling)
    return (root_forward, root_solution, front_solution, subtree_update)


def solution(mesh):
    finer = Mesh(mesh.devices.reshape(8, 4, 2, mesh.shape["panel"]), ("z", "y", "c", "x"))
    in_specs = (
        P(None, "x", LEAF),
        P("x", LEAF, None),
        P("x", LEAF),
        P("x", LEAF),
        P(None, "x", LEAF),
        P("x", None, LEAF),
        P("x", LEAF, None),
        P(None, None),
        P(None, "x"),
        P(LEAF, "x"),
    )
    out_specs = (P(None, LEAF), P(None, "x"), P(None, "x", LEAF), P(None, "x", LEAF))
    return jax.shard_map(
        body, mesh=finer, in_specs=in_specs, out_specs=out_specs, check_vma=False
    )
```

```python
import jax
import jax.numpy as jnp
from jax import lax
from jax.experimental import pallas as pl
from jax.experimental.pallas import tpu as pltpu
from jax.sharding import Mesh
from jax.sharding import PartitionSpec as P

LEAF = ("z", "y", "c")
F32, BF16 = jnp.float32, jnp.bfloat16
NT = (((1,), (1,)), ((), ()))
NN = (((1,), (0,)), ((), ()))


def mm(a, b, dims=NN):
    return lax.dot_general(a, b, dims, preferred_element_type=F32)


def smem():
    return pl.BlockSpec(memory_space=pltpu.SMEM)


def vmem():
    return pl.BlockSpec(memory_space=pltpu.VMEM)


def kernel_call(body, outs, n_smem, n_vmem, flops=0, name=None, near=(), near_out=(), stream=(), far_out=()):
    flat, tree = jax.tree.flatten(outs)
    flat = [pltpu.VMEM(o.shape, o.dtype) if i in near_out else o for i, o in enumerate(flat)]
    call = pl.pallas_call(
        body,
        out_shape=jax.tree.unflatten(tree, flat),
        in_specs=[smem()] * n_smem
        + [vmem()] * n_vmem
        + [pl.BlockSpec(memory_space=pl.ANY)] * len(stream),
        out_specs=jax.tree.unflatten(
            tree,
            [pl.BlockSpec(memory_space=pl.ANY) if i in far_out else vmem() for i in range(len(flat))],
        ),
        scratch_shapes=[pltpu.VMEM(x, BF16) for x in stream]
        + [pltpu.VMEM(flat[i].shape, flat[i].dtype) for i in far_out]
        + [pltpu.SemaphoreType.DMA] * (2 * len(stream) + len(far_out)),
        cost_estimate=pl.CostEstimate(flops=flops, bytes_accessed=flops // 64, transcendentals=0) if flops else None,
        name=name,
    )

    def run(*args):
        args = list(args)
        for i in near:
            args[n_smem + i] = pltpu.with_memory_space_constraint(args[n_smem + i], pltpu.VMEM)
        return call(*args)

    return run


def like(shape, dtype):
    return jax.ShapeDtypeStruct(shape, dtype)


def first_second(c, mine, theirs):
    return jnp.where(c == 0, mine, theirs), jnp.where(c == 0, theirs, mine)


def spread_blocks(both, rows, core, out):
    batch = both.shape[0] // 2
    iota = lax.broadcasted_iota(jnp.int32, (128, 128), 0)
    for block in range(out.shape[0]):
        hot = jnp.where(iota == rows - (block * 256 + core * 128), 1.0, 0.0).astype(BF16)
        spread = mm(both, hot, NT)
        out[block] = (spread[:batch] + spread[batch:]).astype(out.dtype)


def scatter_send_kernel(solved, coupling, sub_map, count, send, both, live_rows):
    contrib = mm(solved[...], coupling[...], NT)
    lane = lax.broadcasted_iota(jnp.int32, (1, 128), 1)
    live = lane < count[...]
    contrib = jnp.where(live, contrib, 0.0)
    high = contrib.astype(BF16)
    low = (contrib - high.astype(F32)).astype(BF16)
    parts = jnp.concatenate([high, low], axis=0)
    rows = jnp.where(live, sub_map[...], -1)
    both[...] = parts
    live_rows[...] = rows
    spread_blocks(parts, rows, 1 - lax.axis_index("c"), send)


def scatter_keep_kernel(both, live_rows, keep):
    spread_blocks(both[...], live_rows[...], lax.axis_index("c"), keep)


def forward_kernel(arrived, rhs, slab, keep, send):
    c = lax.axis_index("c")
    total = jnp.sum(arrived[...].astype(F32), axis=0)
    assembled = (rhs[...] - total).astype(BF16)
    for block in range(keep.shape[0]):
        part = mm(assembled, slab[block * 256 : (block + 1) * 256, :], NT)
        first, second = part[:, :128], part[:, 128:]
        keep[block] = jnp.where(c == 0, first, second)
        send[block] = jnp.where(c == 0, second, first).astype(BF16)


def fold_kernel(base, border, columns, out):
    width = 256
    cols = columns[...]
    lane = lax.broadcasted_iota(jnp.int32, (1, 128), 1)
    left = border[...]
    for block in range(out.shape[1] // width):
        start = base + block * width
        halves = [
            jnp.where(cols == lane + (start + half * 128), 1.0, 0.0).astype(BF16)
            for half in range(width // 128)
        ]
        hot = jnp.concatenate(halves, axis=1)
        out[:, block * width : (block + 1) * width] = mm(left, hot).astype(BF16)


def half_copies(source, buffer, sems):
    width = source.shape[1] // 2
    return [
        pltpu.make_async_copy(
            source.at[:, pl.ds(i * width, width)], buffer.at[:, pl.ds(i * width, width)], sem
        )
        for i, sem in enumerate(sems)
    ]


def border_kernel(arrived, early, source, forward, keep, send, late, *sems):
    c = lax.axis_index("c")
    width = keep.shape[2]
    copies = half_copies(source, late, sems)
    for copy in copies:
        copy.start()
    total = jnp.sum(arrived[...].astype(F32), axis=0)
    forward[...] = total
    half = total.astype(BF16)
    for x in range(4):
        if x >= 2:
            copies[x - 2].wait()
        for y in range(4):
            at = (x % 2 * 4 + y) * width
            part = mm(half, (early, late)[x // 2][:, at : at + width])
            first, second = part[:16], part[16:]
            keep[y * 4 + x] = jnp.where(c == 0, first, second).astype(BF16)
            send[y * 4 + x] = jnp.where(c == 0, second, first).astype(BF16)


def load_kernel(*refs):
    n = len(refs) // 3
    copies = [pltpu.make_async_copy(*each) for each in zip(refs[:n], refs[n : 2 * n], refs[2 * n :])]
    for copy in copies:
        copy.start()
    for copy in copies:
        copy.wait()


def loaded_beside(first, last, arrays, name):
    first, *arrays = lax.optimization_barrier((first, *arrays))
    other = last(first)
    outs = [pltpu.VMEM(a.shape, a.dtype) for a in arrays]
    near = pl.pallas_call(
        load_kernel,
        out_shape=outs,
        in_specs=[pl.BlockSpec(memory_space=pl.ANY)] * len(arrays),
        out_specs=[vmem()] * len(arrays),
        scratch_shapes=[pltpu.SemaphoreType.DMA] * len(arrays),
        cost_estimate=pl.CostEstimate(flops=1 << 30, bytes_accessed=1 << 22, transcendentals=0),
        name=name,
    )(*arrays)
    return first, *lax.optimization_barrier((other, *near))


def pick(index, items):
    out = items[0]
    for k, item in enumerate(items[1:], 1):
        out = jnp.where(index == k, item, out)
    return out


def root_forward_kernel(whole, mine, theirs, out):
    width = whole.shape[2]
    for k, inverse in enumerate((mine, theirs)):
        total = None
        for y in range(4):
            part = mm(whole[y], inverse[:, y * width : (y + 1) * width], NT)
            total = part if total is None else total + part
        out[k] = total


def root_back_kernel(p0, p1, p2, p3, mine, theirs, forward, out):
    x = lax.axis_index("x")
    parts = (p0[...], p1[...], p2[...], p3[...])
    total = None
    for panel in range(4):
        part = pick(lax.rem(x - panel + 4, 4), parts)
        total = part if total is None else total + part
    forward[...] = total
    half = total.astype(BF16)
    width = out.shape[2]
    for y in range(4):
        cols = slice(y * width, (y + 1) * width)
        out[y] = (mm(half[0], mine[:, cols]) + mm(half[1], theirs[:, cols])).astype(BF16)


def residual_kernel(own, other, forward, early, source, residual, far, late, solution, *sems):
    c, x_at = lax.axis_index("c"), lax.axis_index("x")
    width = own.shape[2]
    copies = half_copies(source, late, sems[:2])
    for copy in copies:
        copy.start()
    for y in range(4):
        first, second = first_second(c, own[y * 4 + x_at], other[y * 4 + x_at])
        cols = slice(y * width, (y + 1) * width)
        solution[:16, cols] = first.astype(F32)
        solution[16:, cols] = second.astype(F32)
    out_copy = pltpu.make_async_copy(solution, far, sems[2])
    out_copy.start()
    total = None
    for x in range(4):
        if x >= 2:
            copies[x - 2].wait()
        for y in range(4):
            left = jnp.concatenate(first_second(c, own[y * 4 + x], other[y * 4 + x]), axis=0)
            at = (x % 2 * 4 + y) * width
            part = mm(left, (early, late)[x // 2][:, at : at + width], NT)
            total = part if total is None else total + part
    residual[...] = (forward[...] - total).astype(BF16)
    out_copy.wait()


def front_kernel(own, other, slab, out, half):
    c = lax.axis_index("c")
    total = None
    for block in range(own.shape[0]):
        left = jnp.concatenate(first_second(c, own[block], other[block]), axis=1)
        part = mm(left, slab[block * 256 : (block + 1) * 256, :])
        total = part if total is None else total + part
    out[:, 0, :] = total
    half[...] = total.astype(BF16)


def update_kernel(own, other, live_rows, coupling, ours, later, front, out, far, far_front, forward, copied, *sems):
    c = lax.axis_index("c")
    first, second = first_second(c, ours[0], later[...])
    forward[:16, :] = first
    forward[16:, :] = second
    copied[...] = front[...]
    copies = [
        pltpu.make_async_copy(forward, far, sems[0]),
        pltpu.make_async_copy(copied, far_front, sems[1]),
    ]
    for copy in copies:
        copy.start()
    rows = live_rows[...]
    iota = lax.broadcasted_iota(jnp.int32, (256, 128), 0)
    total = None
    for block in range(own.shape[0]):
        left = jnp.concatenate(first_second(c, own[block], other[block]), axis=1)
        hot = jnp.where(iota == rows - block * 256, 1.0, 0.0).astype(BF16)
        part = mm(left, hot)
        total = part if total is None else total + part
    out[:, 0, :] = mm(total.astype(BF16), coupling[...])
    for copy in copies:
        copy.wait()


def swap_core(x):
    return lax.ppermute(x, "c", [(0, 1), (1, 0)])


def shifted(x, axis, k):
    return lax.ppermute(x, axis, [(i, (i + k) % 4) for i in range(4)])


def exchange(x, axes):
    return lax.all_to_all(x, axes, split_axis=0, concat_axis=0, tiled=True)


def to_everyone(x, axes, peers):
    return exchange(jnp.broadcast_to(x, (peers, *x.shape)), axes)


def joined(keep, got):
    return keep.astype(F32) + got.astype(F32)


def body(
    subtree_solution,
    subtree_coupling,
    sub_map,
    sub_count,
    front_rhs,
    sep_inverse,
    border_coupling,
    border_map,
    root_rhs,
    root_inverse,
):
    z_size, y_size = lax.axis_size("z"), lax.axis_size("y")
    peers = z_size * y_size
    c, y, x = lax.axis_index("c"), lax.axis_index("y"), lax.axis_index("x")
    solved = subtree_solution[:, 0, :]
    coupling = subtree_coupling[0]
    slab = sep_inverse[0]
    border = border_coupling[0]
    batch = solved.shape[0]
    split = like((peers, batch, 128), F32), like((peers, batch, 128), BF16)

    own_map = lax.dynamic_index_in_dim(border_map, x, 0, keepdims=False)
    columns = jnp.broadcast_to(own_map[:, None], (own_map.shape[0], 128))
    panel_width = root_rhs.shape[1]
    folded = []
    for pair in range(2):
        call = kernel_call(
            lambda b, k, o, base=pair * 2 * panel_width: fold_kernel(base, b, k, o),
            like((border.shape[0], 2 * panel_width), BF16),
            0,
            2,
            flops=4 * border.shape[0] * border.shape[1] * panel_width,
            name=f"fold{pair}",
        )
        folded.append(call(border, columns))

    send, both, live_rows = kernel_call(
        scatter_send_kernel,
        (split[1], like((2 * batch, 128), BF16), like(sub_map.shape, jnp.int32)),
        0,
        4,
        name="scatter",
        near_out=(0, 1, 2),
    )(solved, coupling, sub_map, sub_count)
    got = swap_core(send)
    keep = kernel_call(
        scatter_keep_kernel, split[0], 0, 2, flops=1 << 29, name="scatterkeep", near=(0, 1), near_out=(0,)
    )(both, live_rows)
    arrived = exchange(joined(keep, got).astype(BF16), ("z", "y"))
    arrived, folded[0] = lax.optimization_barrier((arrived, folded[0]))
    keep, send = kernel_call(
        forward_kernel,
        split,
        0,
        3,
        name="forward",
        near=(0, 1, 2),
        near_out=(0, 1),
    )(arrived, front_rhs[:, 0, :], slab)
    joint = joined(keep, swap_core(send)).astype(BF16)
    joint, mine = lax.optimization_barrier((joint, root_inverse))
    theirs = swap_core(mine)
    arrived = exchange(joint, ("z", "y"))
    arrived, mine, theirs = lax.optimization_barrier((arrived, mine, theirs))

    quarter = panel_width // 4
    forward, keep, send = kernel_call(
        border_kernel,
        (like((batch, 128), F32), like((16, 16, quarter), BF16), like((16, 16, quarter), BF16)),
        0,
        2,
        name="border",
        near=(0, 1),
        near_out=(0, 1, 2),
        stream=[folded[1].shape],
    )(arrived, *folded)
    rhs_part = lax.dynamic_slice(root_rhs, (c * 16, y * quarter), (16, quarter))
    joint = joined(keep, swap_core(send)).astype(BF16)
    joint, rhs_part = lax.optimization_barrier((joint, rhs_part))
    arrived = exchange(joint, ("y", "x"))
    near = arrived.astype(F32).sum(axis=0).astype(BF16)
    border_sum = to_everyone(near, "z", z_size).astype(F32).sum(axis=0)
    chunk = (rhs_part - border_sum).astype(BF16)
    whole = to_everyone(chunk, "y", y_size)
    pair = like((2, 16, root_inverse.shape[0]), F32)
    partial = kernel_call(
        root_forward_kernel, pair, 0, 3, name="rootf", near=(0, 1, 2), near_out=(0,)
    )(whole, mine, theirs)

    parts = [partial] + [shifted(partial, "x", k) for k in (1, 2, 3)]
    forward_pair, col = kernel_call(
        root_back_kernel,
        (pair, like((4, 16, quarter), BF16)),
        0,
        6,
        name="rootb",
        near=(0, 1, 2, 3, 4, 5),
        near_out=(0, 1),
    )(*parts, mine, theirs)
    near = exchange(col, "y").astype(F32).sum(axis=0).astype(BF16)
    chunk = to_everyone(near, "z", z_size).astype(F32).sum(axis=0).astype(BF16)
    own = to_everyone(chunk, ("y", "x"), 16)
    own, other, near_fold = loaded_beside(own, swap_core, folded[:1], "loadfold")
    residual, root_solution = kernel_call(
        residual_kernel,
        (like((batch, 128), BF16), like((batch, panel_width), F32)),
        0,
        4,
        name="resid",
        near=(0, 1, 2, 3),
        near_out=(0,),
        stream=[folded[1].shape],
        far_out=(1,),
    )(own, other, forward, near_fold, folded[1])

    own = to_everyone(residual, ("z", "y"), peers)
    own, forward_pair = lax.optimization_barrier((own, forward_pair))
    later = swap_core(forward_pair[1])
    own, other, near_slab = loaded_beside(own, swap_core, [slab], "loadslab")
    other, later = lax.optimization_barrier((other, later))
    front, front_half = kernel_call(
        front_kernel,
        (like((batch, 1, 128), F32), like((batch, 128), BF16)),
        0,
        3,
        name="front",
        near=(0, 1, 2),
        near_out=(0, 1),
    )(own, other, near_slab)
    own = to_everyone(front_half, ("z", "y"), peers)
    own, other, near_coupling = loaded_beside(own, swap_core, [coupling], "loadcoup")
    subtree_update, root_forward, front_solution = kernel_call(
        update_kernel,
        (
            like((batch, 1, coupling.shape[1]), F32),
            like((batch, root_inverse.shape[0]), F32),
            like((batch, 1, 128), F32),
        ),
        0,
        7,
        name="update",
        near=tuple(range(7)),
        far_out=(1, 2),
    )(own, other, live_rows, near_coupling, forward_pair, later, front)
    return (root_forward, root_solution, front_solution, subtree_update)


def solution(mesh):
    finer = Mesh(mesh.devices.reshape(8, 4, 2, mesh.shape["panel"]), ("z", "y", "c", "x"))
    in_specs = (
        P(None, "x", LEAF),
        P("x", LEAF, None),
        P("x", LEAF),
        P("x", LEAF),
        P(None, "x", LEAF),
        P("x", None, LEAF),
        P("x", LEAF, None),
        P(None, None),
        P(None, "x"),
        P(LEAF, "x"),
    )
    out_specs = (P(None, LEAF), P(None, "x"), P(None, "x", LEAF), P(None, "x", LEAF))
    return jax.shard_map(
        body, mesh=finer, in_specs=in_specs, out_specs=out_specs, check_vma=False
    )
```

```python
import jax
import jax.numpy as jnp
from jax import lax
from jax.experimental import pallas as pl
from jax.experimental.pallas import tpu as pltpu
from jax.sharding import Mesh
from jax.sharding import PartitionSpec as P

LEAF = ("z", "y", "c")
F32, BF16 = jnp.float32, jnp.bfloat16
NT = (((1,), (1,)), ((), ()))
NN = (((1,), (0,)), ((), ()))


def mm(a, b, dims=NN):
    return lax.dot_general(a, b, dims, preferred_element_type=F32)


def smem():
    return pl.BlockSpec(memory_space=pltpu.SMEM)


def vmem():
    return pl.BlockSpec(memory_space=pltpu.VMEM)


def kernel_call(body, outs, n_smem, n_vmem, flops=0, name=None, near=(), near_out=(), stream=(), far_out=(), more_sems=0):
    flat, tree = jax.tree.flatten(outs)
    flat = [pltpu.VMEM(o.shape, o.dtype) if i in near_out else o for i, o in enumerate(flat)]
    call = pl.pallas_call(
        body,
        out_shape=jax.tree.unflatten(tree, flat),
        in_specs=[smem()] * n_smem
        + [vmem()] * n_vmem
        + [pl.BlockSpec(memory_space=pl.ANY)] * len(stream),
        out_specs=jax.tree.unflatten(
            tree,
            [pl.BlockSpec(memory_space=pl.ANY) if i in far_out else vmem() for i in range(len(flat))],
        ),
        scratch_shapes=[pltpu.VMEM(x, BF16) for x in stream]
        + [pltpu.VMEM(flat[i].shape, flat[i].dtype) for i in far_out]
        + [pltpu.SemaphoreType.DMA] * (2 * len(stream) + len(far_out) + more_sems),
        cost_estimate=pl.CostEstimate(flops=flops, bytes_accessed=flops // 64, transcendentals=0) if flops else None,
        name=name,
    )

    def run(*args):
        args = list(args)
        for i in near:
            args[n_smem + i] = pltpu.with_memory_space_constraint(args[n_smem + i], pltpu.VMEM)
        return call(*args)

    return run


def like(shape, dtype):
    return jax.ShapeDtypeStruct(shape, dtype)


def first_second(c, mine, theirs):
    return jnp.where(c == 0, mine, theirs), jnp.where(c == 0, theirs, mine)


def contribution_kernel(solved, coupling, sub_map, count, packed):
    contrib = mm(solved[...], coupling[...], NT)
    lane = lax.broadcasted_iota(jnp.int32, (1, 128), 1)
    live = lane < count[...]
    rows = jnp.where(live, sub_map[...], -1)
    batch = contrib.shape[0]
    packed[:batch] = jnp.where(live, contrib, 0.0)
    packed[batch:] = jnp.broadcast_to(rows.astype(F32), (packed.shape[0] - batch, 128))


def scatter_kernel(own, other, out, far, live_rows, sem):
    c = lax.axis_index("c")
    batch = out.shape[1]
    live_rows[...] = own[batch : batch + 1].astype(jnp.int32)
    copy = pltpu.make_async_copy(live_rows, far, sem)
    copy.start()
    values = jnp.concatenate([own[:batch], other[:batch]], axis=1)
    rows = jnp.concatenate([own[batch : batch + 1], other[batch : batch + 1]], axis=1)
    rows = rows.astype(jnp.int32)
    high = values.astype(BF16)
    low = (values - high.astype(F32)).astype(BF16)
    both = jnp.concatenate([high, low], axis=0)
    iota = lax.broadcasted_iota(jnp.int32, (128, 256), 0)
    for block in range(out.shape[0]):
        hot = jnp.where(iota == rows - (block * 256 + c * 128), 1.0, 0.0).astype(BF16)
        spread = mm(both, hot, NT)
        out[block] = (spread[:batch] + spread[batch:]).astype(BF16)
    copy.wait()


def forward_kernel(arrived, rhs, slab, keep, send):
    c = lax.axis_index("c")
    total = jnp.sum(arrived[...].astype(F32), axis=0)
    assembled = (rhs[...] - total).astype(BF16)
    for block in range(keep.shape[0]):
        part = mm(assembled, slab[block * 256 : (block + 1) * 256, :], NT)
        first, second = part[:, :128], part[:, 128:]
        keep[block] = jnp.where(c == 0, first, second)
        send[block] = jnp.where(c == 0, second, first).astype(BF16)


def fold_kernel(base, border, columns, out):
    width = 256
    cols = columns[...]
    lane = lax.broadcasted_iota(jnp.int32, (1, 128), 1)
    left = border[...]
    for block in range(out.shape[1] // width):
        start = base + block * width
        halves = [
            jnp.where(cols == lane + (start + half * 128), 1.0, 0.0).astype(BF16)
            for half in range(width // 128)
        ]
        hot = jnp.concatenate(halves, axis=1)
        out[:, block * width : (block + 1) * width] = mm(left, hot).astype(BF16)


def half_copies(source, buffer, sems):
    width = source.shape[1] // 2
    return [
        pltpu.make_async_copy(
            source.at[:, pl.ds(i * width, width)], buffer.at[:, pl.ds(i * width, width)], sem
        )
        for i, sem in enumerate(sems)
    ]


def border_kernel(arrived, early, source, forward, keep, send, late, *sems):
    c = lax.axis_index("c")
    width = keep.shape[2]
    copies = half_copies(source, late, sems)
    for copy in copies:
        copy.start()
    total = jnp.sum(arrived[...].astype(F32), axis=0)
    forward[...] = total
    half = total.astype(BF16)
    for x in range(4):
        if x >= 2:
            copies[x - 2].wait()
        for y in range(4):
            at = (x % 2 * 4 + y) * width
            part = mm(half, (early, late)[x // 2][:, at : at + width])
            first, second = part[:16], part[16:]
            keep[y * 4 + x] = jnp.where(c == 0, first, second).astype(BF16)
            send[y * 4 + x] = jnp.where(c == 0, second, first).astype(BF16)


def load_kernel(*refs):
    n = len(refs) // 3
    copies = [pltpu.make_async_copy(*each) for each in zip(refs[:n], refs[n : 2 * n], refs[2 * n :])]
    for copy in copies:
        copy.start()
    for copy in copies:
        copy.wait()


def loaded_beside(first, last, arrays, name):
    first, *arrays = lax.optimization_barrier((first, *arrays))
    other = last(first)
    outs = [pltpu.VMEM(a.shape, a.dtype) for a in arrays]
    near = pl.pallas_call(
        load_kernel,
        out_shape=outs,
        in_specs=[pl.BlockSpec(memory_space=pl.ANY)] * len(arrays),
        out_specs=[vmem()] * len(arrays),
        scratch_shapes=[pltpu.SemaphoreType.DMA] * len(arrays),
        cost_estimate=pl.CostEstimate(flops=1 << 30, bytes_accessed=1 << 22, transcendentals=0),
        name=name,
    )(*arrays)
    return first, *lax.optimization_barrier((other, *near))


def pick(index, items):
    out = items[0]
    for k, item in enumerate(items[1:], 1):
        out = jnp.where(index == k, item, out)
    return out


def root_forward_kernel(whole, mine, theirs, out):
    width = whole.shape[2]
    for k, inverse in enumerate((mine, theirs)):
        total = None
        for y in range(4):
            part = mm(whole[y], inverse[:, y * width : (y + 1) * width], NT)
            total = part if total is None else total + part
        out[k] = total


def root_back_kernel(p0, p1, p2, p3, mine, theirs, forward, out):
    x = lax.axis_index("x")
    parts = (p0[...], p1[...], p2[...], p3[...])
    total = None
    for panel in range(4):
        part = pick(lax.rem(x - panel + 4, 4), parts)
        total = part if total is None else total + part
    forward[...] = total
    half = total.astype(BF16)
    width = out.shape[2]
    for y in range(4):
        cols = slice(y * width, (y + 1) * width)
        out[y] = (mm(half[0], mine[:, cols]) + mm(half[1], theirs[:, cols])).astype(BF16)


def residual_kernel(own, other, forward, early, source, residual, far, late, solution, *sems):
    c, x_at = lax.axis_index("c"), lax.axis_index("x")
    width = own.shape[2]
    copies = half_copies(source, late, sems[:2])
    for copy in copies:
        copy.start()
    for y in range(4):
        first, second = first_second(c, own[y * 4 + x_at], other[y * 4 + x_at])
        cols = slice(y * width, (y + 1) * width)
        solution[:16, cols] = first.astype(F32)
        solution[16:, cols] = second.astype(F32)
    out_copy = pltpu.make_async_copy(solution, far, sems[2])
    out_copy.start()
    total = None
    for x in range(4):
        if x >= 2:
            copies[x - 2].wait()
        for y in range(4):
            left = jnp.concatenate(first_second(c, own[y * 4 + x], other[y * 4 + x]), axis=0)
            at = (x % 2 * 4 + y) * width
            part = mm(left, (early, late)[x // 2][:, at : at + width], NT)
            total = part if total is None else total + part
    residual[...] = (forward[...] - total).astype(BF16)
    out_copy.wait()


def front_kernel(own, other, slab, out, half):
    c = lax.axis_index("c")
    total = None
    for block in range(own.shape[0]):
        left = jnp.concatenate(first_second(c, own[block], other[block]), axis=1)
        part = mm(left, slab[block * 256 : (block + 1) * 256, :])
        total = part if total is None else total + part
    out[:, 0, :] = total
    half[...] = total.astype(BF16)


def update_kernel(own, other, live_rows, coupling, ours, later, front, far_out, far, far_front, out, forward, copied, *sems):
    c = lax.axis_index("c")
    first, second = first_second(c, ours[0], later[...])
    forward[:16, :] = first
    forward[16:, :] = second
    copied[...] = front[...]
    copies = [
        pltpu.make_async_copy(forward, far, sems[0]),
        pltpu.make_async_copy(copied, far_front, sems[1]),
    ]
    for copy in copies:
        copy.start()
    rows = live_rows[...]
    iota = lax.broadcasted_iota(jnp.int32, (256, 128), 0)
    total = None
    for block in range(own.shape[0]):
        left = jnp.concatenate(first_second(c, own[block], other[block]), axis=1)
        hot = jnp.where(iota == rows - block * 256, 1.0, 0.0).astype(BF16)
        part = mm(left, hot)
        total = part if total is None else total + part
    picked = total.astype(BF16)
    width = out.shape[2] // 2
    for k in range(2):
        cols = pl.ds(k * width, width)
        out[:, 0, k * width : (k + 1) * width] = mm(picked, coupling[:, k * width : (k + 1) * width])
        copies.append(pltpu.make_async_copy(out.at[:, :, cols], far_out.at[:, :, cols], sems[2 + k]))
        copies[-1].start()
    for copy in copies:
        copy.wait()


def swap_core(x):
    return lax.ppermute(x, "c", [(0, 1), (1, 0)])


def shifted(x, axis, k):
    return lax.ppermute(x, axis, [(i, (i + k) % 4) for i in range(4)])


def exchange(x, axes):
    return lax.all_to_all(x, axes, split_axis=0, concat_axis=0, tiled=True)


def to_everyone(x, axes, peers):
    return exchange(jnp.broadcast_to(x, (peers, *x.shape)), axes)


def joined(keep, got):
    return keep.astype(F32) + got.astype(F32)


def body(
    subtree_solution,
    subtree_coupling,
    sub_map,
    sub_count,
    front_rhs,
    sep_inverse,
    border_coupling,
    border_map,
    root_rhs,
    root_inverse,
):
    z_size, y_size = lax.axis_size("z"), lax.axis_size("y")
    peers = z_size * y_size
    c, y, x = lax.axis_index("c"), lax.axis_index("y"), lax.axis_index("x")
    solved = subtree_solution[:, 0, :]
    coupling = subtree_coupling[0]
    slab = sep_inverse[0]
    border = border_coupling[0]
    batch = solved.shape[0]
    split = like((peers, batch, 128), F32), like((peers, batch, 128), BF16)

    own_map = lax.dynamic_index_in_dim(border_map, x, 0, keepdims=False)
    columns = jnp.broadcast_to(own_map[:, None], (own_map.shape[0], 128))
    panel_width = root_rhs.shape[1]
    folded = []
    for pair in range(2):
        call = kernel_call(
            lambda b, k, o, base=pair * 2 * panel_width: fold_kernel(base, b, k, o),
            like((border.shape[0], 2 * panel_width), BF16),
            0,
            2,
            flops=4 * border.shape[0] * border.shape[1] * panel_width,
            name=f"fold{pair}",
        )
        folded.append(call(border, columns))

    packed = kernel_call(
        contribution_kernel, like((batch + 8, 128), F32), 0, 4, name="contrib", near_out=(0,)
    )(solved, coupling, sub_map, sub_count)
    spread, live_rows = kernel_call(
        scatter_kernel,
        (split[1], like(sub_map.shape, jnp.int32)),
        0,
        2,
        name="scatter",
        near=(0, 1),
        far_out=(1,),
    )(packed, swap_core(packed))
    arrived = exchange(spread, ("z", "y"))
    arrived, folded[0] = lax.optimization_barrier((arrived, folded[0]))
    keep, send = kernel_call(
        forward_kernel,
        split,
        0,
        3,
        name="forward",
        near=(0, 1, 2),
        near_out=(0, 1),
    )(arrived, front_rhs[:, 0, :], slab)
    joint = joined(keep, swap_core(send)).astype(BF16)
    joint, mine = lax.optimization_barrier((joint, root_inverse))
    theirs = swap_core(mine)
    arrived = exchange(joint, ("z", "y"))
    arrived, mine, theirs = lax.optimization_barrier((arrived, mine, theirs))

    quarter = panel_width // 4
    forward, keep, send = kernel_call(
        border_kernel,
        (like((batch, 128), F32), like((16, 16, quarter), BF16), like((16, 16, quarter), BF16)),
        0,
        2,
        name="border",
        near=(0, 1),
        near_out=(0, 1, 2),
        stream=[folded[1].shape],
    )(arrived, *folded)
    rhs_part = lax.dynamic_slice(root_rhs, (c * 16, y * quarter), (16, quarter))
    joint = joined(keep, swap_core(send)).astype(BF16)
    joint, rhs_part = lax.optimization_barrier((joint, rhs_part))
    arrived = exchange(joint, ("y", "x"))
    near = arrived.astype(F32).sum(axis=0).astype(BF16)
    border_sum = to_everyone(near, "z", z_size).astype(F32).sum(axis=0)
    chunk = (rhs_part - border_sum).astype(BF16)
    whole = to_everyone(chunk, "y", y_size)
    pair = like((2, 16, root_inverse.shape[0]), F32)
    partial = kernel_call(
        root_forward_kernel, pair, 0, 3, name="rootf", near=(0, 1, 2), near_out=(0,)
    )(whole, mine, theirs)

    parts = [partial] + [shifted(partial, "x", k) for k in (1, 2, 3)]
    forward_pair, col = kernel_call(
        root_back_kernel,
        (pair, like((4, 16, quarter), BF16)),
        0,
        6,
        name="rootb",
        near=(0, 1, 2, 3, 4, 5),
        near_out=(0, 1),
    )(*parts, mine, theirs)
    near = exchange(col, "y").astype(F32).sum(axis=0).astype(BF16)
    chunk = to_everyone(near, "z", z_size).astype(F32).sum(axis=0).astype(BF16)
    own = to_everyone(chunk, ("y", "x"), 16)
    own, other, near_fold = loaded_beside(own, swap_core, folded[:1], "loadfold")
    residual, root_solution = kernel_call(
        residual_kernel,
        (like((batch, 128), BF16), like((batch, panel_width), F32)),
        0,
        4,
        name="resid",
        near=(0, 1, 2, 3),
        near_out=(0,),
        stream=[folded[1].shape],
        far_out=(1,),
    )(own, other, forward, near_fold, folded[1])

    own = to_everyone(residual, ("z", "y"), peers)
    own, forward_pair = lax.optimization_barrier((own, forward_pair))
    later = swap_core(forward_pair[1])
    own, other, near_slab = loaded_beside(own, swap_core, [slab], "loadslab")
    other, later = lax.optimization_barrier((other, later))
    front, front_half = kernel_call(
        front_kernel,
        (like((batch, 1, 128), F32), like((batch, 128), BF16)),
        0,
        3,
        name="front",
        near=(0, 1, 2),
        near_out=(0, 1),
    )(own, other, near_slab)
    own = to_everyone(front_half, ("z", "y"), peers)
    own, other, near_coupling = loaded_beside(own, swap_core, [coupling], "loadcoup")
    subtree_update, root_forward, front_solution = kernel_call(
        update_kernel,
        (
            like((batch, 1, coupling.shape[1]), F32),
            like((batch, root_inverse.shape[0]), F32),
            like((batch, 1, 128), F32),
        ),
        0,
        7,
        name="update",
        near=tuple(range(7)),
        far_out=(0, 1, 2),
        more_sems=1,
    )(own, other, live_rows, near_coupling, forward_pair, later, front)
    return (root_forward, root_solution, front_solution, subtree_update)


def solution(mesh):
    finer = Mesh(mesh.devices.reshape(8, 4, 2, mesh.shape["panel"]), ("z", "y", "c", "x"))
    in_specs = (
        P(None, "x", LEAF),
        P("x", LEAF, None),
        P("x", LEAF),
        P("x", LEAF),
        P(None, "x", LEAF),
        P("x", None, LEAF),
        P("x", LEAF, None),
        P(None, None),
        P(None, "x"),
        P(LEAF, "x"),
    )
    out_specs = (P(None, LEAF), P(None, "x"), P(None, "x", LEAF), P(None, "x", LEAF))
    return jax.shard_map(
        body, mesh=finer, in_specs=in_specs, out_specs=out_specs, check_vma=False
    )
```

```python
import jax
import jax.numpy as jnp
from jax import lax
from jax.experimental import pallas as pl
from jax.experimental.pallas import tpu as pltpu
from jax.sharding import Mesh
from jax.sharding import PartitionSpec as P

LEAF = ("z", "y", "c")
F32, BF16 = jnp.float32, jnp.bfloat16
NT = (((1,), (1,)), ((), ()))
NN = (((1,), (0,)), ((), ()))


def mm(a, b, dims=NN):
    return lax.dot_general(a, b, dims, preferred_element_type=F32)


def smem():
    return pl.BlockSpec(memory_space=pltpu.SMEM)


def vmem():
    return pl.BlockSpec(memory_space=pltpu.VMEM)


def kernel_call(body, outs, n_smem, n_vmem, flops=0, name=None, near=(), near_out=(), stream=(), far_out=(), more_sems=0):
    flat, tree = jax.tree.flatten(outs)
    flat = [pltpu.VMEM(o.shape, o.dtype) if i in near_out else o for i, o in enumerate(flat)]
    call = pl.pallas_call(
        body,
        out_shape=jax.tree.unflatten(tree, flat),
        in_specs=[smem()] * n_smem
        + [vmem()] * n_vmem
        + [pl.BlockSpec(memory_space=pl.ANY)] * len(stream),
        out_specs=jax.tree.unflatten(
            tree,
            [pl.BlockSpec(memory_space=pl.ANY) if i in far_out else vmem() for i in range(len(flat))],
        ),
        scratch_shapes=[pltpu.VMEM(x, BF16) for x in stream]
        + [pltpu.VMEM(flat[i].shape, flat[i].dtype) for i in far_out]
        + [pltpu.SemaphoreType.DMA] * (2 * len(stream) + len(far_out) + more_sems),
        cost_estimate=pl.CostEstimate(flops=flops, bytes_accessed=flops // 64, transcendentals=0) if flops else None,
        name=name,
    )

    def run(*args):
        args = list(args)
        for i in near:
            args[n_smem + i] = pltpu.with_memory_space_constraint(args[n_smem + i], pltpu.VMEM)
        return call(*args)

    return run


def like(shape, dtype):
    return jax.ShapeDtypeStruct(shape, dtype)


def first_second(c, mine, theirs):
    return jnp.where(c == 0, mine, theirs), jnp.where(c == 0, theirs, mine)


def contribution_kernel(solved, coupling, sub_map, count, packed):
    contrib = mm(solved[...], coupling[...], NT)
    lane = lax.broadcasted_iota(jnp.int32, (1, 128), 1)
    live = lane < count[...]
    rows = jnp.where(live, sub_map[...], -1)
    batch = contrib.shape[0]
    packed[:batch] = jnp.where(live, contrib, 0.0)
    packed[batch:] = jnp.broadcast_to(rows.astype(F32), (packed.shape[0] - batch, 128))


def scatter_kernel(own, other, far_out, far, out, live_rows, *sems):
    c = lax.axis_index("c")
    batch = out.shape[1]
    live_rows[...] = own[batch : batch + 1].astype(jnp.int32)
    copies = [pltpu.make_async_copy(live_rows, far, sems[0])]
    copies[0].start()
    values = jnp.concatenate([own[:batch], other[:batch]], axis=1)
    rows = jnp.concatenate([own[batch : batch + 1], other[batch : batch + 1]], axis=1)
    rows = rows.astype(jnp.int32)
    high = values.astype(BF16)
    low = (values - high.astype(F32)).astype(BF16)
    both = jnp.concatenate([high, low], axis=0)
    iota = lax.broadcasted_iota(jnp.int32, (128, 256), 0)
    for block in range(out.shape[0]):
        hot = jnp.where(iota == rows - (block * 256 + c * 128), 1.0, 0.0).astype(BF16)
        spread = mm(both, hot, NT)
        out[block] = (spread[:batch] + spread[batch:]).astype(BF16)
        if block % 8 == 7:
            done = pl.ds(block - 7, 8)
            copies.append(
                pltpu.make_async_copy(out.at[done], far_out.at[done], sems[1 + block // 8])
            )
            copies[-1].start()
    for copy in copies:
        copy.wait()


def forward_kernel(arrived, rhs, slab, keep, send):
    c = lax.axis_index("c")
    total = jnp.sum(arrived[...].astype(F32), axis=0)
    assembled = (rhs[...] - total).astype(BF16)
    for block in range(keep.shape[0]):
        part = mm(assembled, slab[block * 256 : (block + 1) * 256, :], NT)
        first, second = part[:, :128], part[:, 128:]
        keep[block] = jnp.where(c == 0, first, second)
        send[block] = jnp.where(c == 0, second, first).astype(BF16)


def fold_kernel(base, border, columns, out):
    width = 256
    cols = columns[...]
    lane = lax.broadcasted_iota(jnp.int32, (1, 128), 1)
    left = border[...]
    for block in range(out.shape[1] // width):
        start = base + block * width
        halves = [
            jnp.where(cols == lane + (start + half * 128), 1.0, 0.0).astype(BF16)
            for half in range(width // 128)
        ]
        hot = jnp.concatenate(halves, axis=1)
        out[:, block * width : (block + 1) * width] = mm(left, hot).astype(BF16)


def half_copies(source, buffer, sems):
    width = source.shape[1] // 2
    return [
        pltpu.make_async_copy(
            source.at[:, pl.ds(i * width, width)], buffer.at[:, pl.ds(i * width, width)], sem
        )
        for i, sem in enumerate(sems)
    ]


def border_kernel(arrived, early, source, forward, keep, send, late, *sems):
    c = lax.axis_index("c")
    width = keep.shape[2]
    copies = half_copies(source, late, sems)
    for copy in copies:
        copy.start()
    total = jnp.sum(arrived[...].astype(F32), axis=0)
    forward[...] = total
    half = total.astype(BF16)
    for x in range(4):
        if x >= 2:
            copies[x - 2].wait()
        for y in range(4):
            at = (x % 2 * 4 + y) * width
            part = mm(half, (early, late)[x // 2][:, at : at + width])
            first, second = part[:16], part[16:]
            keep[y * 4 + x] = jnp.where(c == 0, first, second).astype(BF16)
            send[y * 4 + x] = jnp.where(c == 0, second, first).astype(BF16)


def load_kernel(*refs):
    n = len(refs) // 3
    copies = [pltpu.make_async_copy(*each) for each in zip(refs[:n], refs[n : 2 * n], refs[2 * n :])]
    for copy in copies:
        copy.start()
    for copy in copies:
        copy.wait()


def loaded_beside(first, last, arrays, name):
    first, *arrays = lax.optimization_barrier((first, *arrays))
    other = last(first)
    outs = [pltpu.VMEM(a.shape, a.dtype) for a in arrays]
    near = pl.pallas_call(
        load_kernel,
        out_shape=outs,
        in_specs=[pl.BlockSpec(memory_space=pl.ANY)] * len(arrays),
        out_specs=[vmem()] * len(arrays),
        scratch_shapes=[pltpu.SemaphoreType.DMA] * len(arrays),
        cost_estimate=pl.CostEstimate(flops=1 << 30, bytes_accessed=1 << 22, transcendentals=0),
        name=name,
    )(*arrays)
    return first, *lax.optimization_barrier((other, *near))


def pick(index, items):
    out = items[0]
    for k, item in enumerate(items[1:], 1):
        out = jnp.where(index == k, item, out)
    return out


def root_forward_kernel(whole, mine, theirs, out):
    width = whole.shape[2]
    for k, inverse in enumerate((mine, theirs)):
        total = None
        for y in range(4):
            part = mm(whole[y], inverse[:, y * width : (y + 1) * width], NT)
            total = part if total is None else total + part
        out[k] = total


def root_back_kernel(p0, p1, p3, p2, mine, theirs, forward, out):
    x = lax.axis_index("x")
    parts = (p0[...], p1[...], p2[...], p3[...])
    total = None
    for panel in range(4):
        part = pick(lax.rem(x - panel + 4, 4), parts)
        total = part if total is None else total + part
    forward[...] = total
    half = total.astype(BF16)
    width = out.shape[2]
    for y in range(4):
        cols = slice(y * width, (y + 1) * width)
        out[y] = (mm(half[0], mine[:, cols]) + mm(half[1], theirs[:, cols])).astype(BF16)


def residual_kernel(own, other, forward, early, source, residual, far, late, solution, *sems):
    c, x_at = lax.axis_index("c"), lax.axis_index("x")
    width = own.shape[2]
    copies = half_copies(source, late, sems[:2])
    for copy in copies:
        copy.start()
    for y in range(4):
        first, second = first_second(c, own[y * 4 + x_at], other[y * 4 + x_at])
        cols = slice(y * width, (y + 1) * width)
        solution[:16, cols] = first.astype(F32)
        solution[16:, cols] = second.astype(F32)
    out_copy = pltpu.make_async_copy(solution, far, sems[2])
    out_copy.start()
    total = None
    for x in range(4):
        if x >= 2:
            copies[x - 2].wait()
        for y in range(4):
            left = jnp.concatenate(first_second(c, own[y * 4 + x], other[y * 4 + x]), axis=0)
            at = (x % 2 * 4 + y) * width
            part = mm(left, (early, late)[x // 2][:, at : at + width], NT)
            total = part if total is None else total + part
    residual[...] = (forward[...] - total).astype(BF16)
    out_copy.wait()


def front_kernel(own, other, slab, out, half):
    c = lax.axis_index("c")
    total = None
    for block in range(own.shape[0]):
        left = jnp.concatenate(first_second(c, own[block], other[block]), axis=1)
        part = mm(left, slab[block * 256 : (block + 1) * 256, :])
        total = part if total is None else total + part
    out[:, 0, :] = total
    half[...] = total.astype(BF16)


def update_kernel(own, other, live_rows, coupling, ours, later, front, far_out, far, far_front, out, forward, copied, *sems):
    c = lax.axis_index("c")
    first, second = first_second(c, ours[0], later[...])
    forward[:16, :] = first
    forward[16:, :] = second
    copied[...] = front[...]
    copies = [
        pltpu.make_async_copy(forward, far, sems[0]),
        pltpu.make_async_copy(copied, far_front, sems[1]),
    ]
    for copy in copies:
        copy.start()
    rows = live_rows[...]
    iota = lax.broadcasted_iota(jnp.int32, (256, 128), 0)
    total = None
    for block in range(own.shape[0]):
        left = jnp.concatenate(first_second(c, own[block], other[block]), axis=1)
        hot = jnp.where(iota == rows - block * 256, 1.0, 0.0).astype(BF16)
        part = mm(left, hot)
        total = part if total is None else total + part
    picked = total.astype(BF16)
    width = out.shape[2] // 2
    for k in range(2):
        cols = pl.ds(k * width, width)
        out[:, 0, k * width : (k + 1) * width] = mm(picked, coupling[:, k * width : (k + 1) * width])
        copies.append(pltpu.make_async_copy(out.at[:, :, cols], far_out.at[:, :, cols], sems[2 + k]))
        copies[-1].start()
    for copy in copies:
        copy.wait()


def swap_core(x):
    return lax.ppermute(x, "c", [(0, 1), (1, 0)])


def shifted(x, axis, k):
    return lax.ppermute(x, axis, [(i, (i + k) % 4) for i in range(4)])


def exchange(x, axes):
    return lax.all_to_all(x, axes, split_axis=0, concat_axis=0, tiled=True)


def to_everyone(x, axes, peers):
    return exchange(jnp.broadcast_to(x, (peers, *x.shape)), axes)


def joined(keep, got):
    return keep.astype(F32) + got.astype(F32)


def body(
    subtree_solution,
    subtree_coupling,
    sub_map,
    sub_count,
    front_rhs,
    sep_inverse,
    border_coupling,
    border_map,
    root_rhs,
    root_inverse,
):
    z_size, y_size = lax.axis_size("z"), lax.axis_size("y")
    peers = z_size * y_size
    c, y, x = lax.axis_index("c"), lax.axis_index("y"), lax.axis_index("x")
    solved = subtree_solution[:, 0, :]
    coupling = subtree_coupling[0]
    slab = sep_inverse[0]
    border = border_coupling[0]
    batch = solved.shape[0]
    split = like((peers, batch, 128), F32), like((peers, batch, 128), BF16)

    own_map = lax.dynamic_index_in_dim(border_map, x, 0, keepdims=False)
    columns = jnp.broadcast_to(own_map[:, None], (own_map.shape[0], 128))
    panel_width = root_rhs.shape[1]
    folded = []
    for pair in range(2):
        call = kernel_call(
            lambda b, k, o, base=pair * 2 * panel_width: fold_kernel(base, b, k, o),
            like((border.shape[0], 2 * panel_width), BF16),
            0,
            2,
            flops=4 * border.shape[0] * border.shape[1] * panel_width,
            name=f"fold{pair}",
        )
        folded.append(call(border, columns))

    packed = kernel_call(
        contribution_kernel, like((batch + 8, 128), F32), 0, 4, name="contrib", near_out=(0,)
    )(solved, coupling, sub_map, sub_count)
    spread, live_rows = kernel_call(
        scatter_kernel,
        (split[1], like(sub_map.shape, jnp.int32)),
        0,
        2,
        name="scatter",
        near=(0, 1),
        far_out=(0, 1),
        more_sems=3,
    )(packed, swap_core(packed))
    arrived = exchange(spread, ("z", "y"))
    arrived, folded[0] = lax.optimization_barrier((arrived, folded[0]))
    keep, send = kernel_call(
        forward_kernel,
        split,
        0,
        3,
        name="forward",
        near=(0, 1, 2),
        near_out=(0, 1),
    )(arrived, front_rhs[:, 0, :], slab)
    joint = joined(keep, swap_core(send)).astype(BF16)
    joint, mine = lax.optimization_barrier((joint, root_inverse))
    theirs = swap_core(mine)
    arrived = exchange(joint, ("z", "y"))
    arrived, mine, theirs = lax.optimization_barrier((arrived, mine, theirs))

    quarter = panel_width // 4
    forward, keep, send = kernel_call(
        border_kernel,
        (like((batch, 128), F32), like((16, 16, quarter), BF16), like((16, 16, quarter), BF16)),
        0,
        2,
        name="border",
        near=(0, 1),
        near_out=(0, 1, 2),
        stream=[folded[1].shape],
    )(arrived, *folded)
    rhs_part = lax.dynamic_slice(root_rhs, (c * 16, y * quarter), (16, quarter))
    joint = joined(keep, swap_core(send)).astype(BF16)
    joint, rhs_part = lax.optimization_barrier((joint, rhs_part))
    arrived = exchange(joint, ("y", "x"))
    near = arrived.astype(F32).sum(axis=0).astype(BF16)
    border_sum = to_everyone(near, "z", z_size).astype(F32).sum(axis=0)
    chunk = (rhs_part - border_sum).astype(BF16)
    whole = to_everyone(chunk, "y", y_size)
    pair = like((2, 16, root_inverse.shape[0]), F32)
    partial = kernel_call(
        root_forward_kernel, pair, 0, 3, name="rootf", near=(0, 1, 2), near_out=(0,)
    )(whole, mine, theirs)

    moved = {k: shifted(partial, "x", k) for k in (1, 3, 2)}
    parts = [partial] + [moved[k] for k in (1, 3, 2)]
    forward_pair, col = kernel_call(
        root_back_kernel,
        (pair, like((4, 16, quarter), BF16)),
        0,
        6,
        name="rootb",
        near=(0, 1, 2, 3, 4, 5),
        near_out=(0, 1),
    )(*parts, mine, theirs)
    near = exchange(col, "y").astype(F32).sum(axis=0).astype(BF16)
    chunk = to_everyone(near, "z", z_size).astype(F32).sum(axis=0).astype(BF16)
    own = to_everyone(chunk, ("y", "x"), 16)
    own, other, near_fold = loaded_beside(own, swap_core, folded[:1], "loadfold")
    residual, root_solution = kernel_call(
        residual_kernel,
        (like((batch, 128), BF16), like((batch, panel_width), F32)),
        0,
        4,
        name="resid",
        near=(0, 1, 2, 3),
        near_out=(0,),
        stream=[folded[1].shape],
        far_out=(1,),
    )(own, other, forward, near_fold, folded[1])

    own = to_everyone(residual, ("z", "y"), peers)
    own, forward_pair = lax.optimization_barrier((own, forward_pair))
    later = swap_core(forward_pair[1])
    own, other, near_slab = loaded_beside(own, swap_core, [slab], "loadslab")
    other, later = lax.optimization_barrier((other, later))
    front, front_half = kernel_call(
        front_kernel,
        (like((batch, 1, 128), F32), like((batch, 128), BF16)),
        0,
        3,
        name="front",
        near=(0, 1, 2),
        near_out=(0, 1),
    )(own, other, near_slab)
    own = to_everyone(front_half, ("z", "y"), peers)
    own, other, near_coupling = loaded_beside(own, swap_core, [coupling], "loadcoup")
    subtree_update, root_forward, front_solution = kernel_call(
        update_kernel,
        (
            like((batch, 1, coupling.shape[1]), F32),
            like((batch, root_inverse.shape[0]), F32),
            like((batch, 1, 128), F32),
        ),
        0,
        7,
        name="update",
        near=tuple(range(7)),
        far_out=(0, 1, 2),
        more_sems=1,
    )(own, other, live_rows, near_coupling, forward_pair, later, front)
    return (root_forward, root_solution, front_solution, subtree_update)


def solution(mesh):
    finer = Mesh(mesh.devices.reshape(8, 4, 2, mesh.shape["panel"]), ("z", "y", "c", "x"))
    in_specs = (
        P(None, "x", LEAF),
        P("x", LEAF, None),
        P("x", LEAF),
        P("x", LEAF),
        P(None, "x", LEAF),
        P("x", None, LEAF),
        P("x", LEAF, None),
        P(None, None),
        P(None, "x"),
        P(LEAF, "x"),
    )
    out_specs = (P(None, LEAF), P(None, "x"), P(None, "x", LEAF), P(None, "x", LEAF))
    return jax.shard_map(
        body, mesh=finer, in_specs=in_specs, out_specs=out_specs, check_vma=False
    )
```
